512 devices in a mesh: frames: 64 (over z, y_hi, core), heads: 8 (over y_lo, x).
Axes of the slice: x: 4, y: 8 (y_hi: 4, y_lo: 2; y = y_hi * 2 + y_lo), z: 8, core: 2. Of those that a mesh axis runs over, the one named last changes fastest.
Arguments:
- queries: bfloat16 [16384, 2048], P('frames', 'heads'), may hold values from -8 to 8
- keys: bfloat16 [16384, 2048], P('frames', 'heads'), may hold values from -8 to 8
- values: bfloat16 [16384, 2048], P('frames', 'heads'), may hold values from -6 to 6
- out_grad: bfloat16 [16384, 2048], P('frames', 'heads'), may hold values from -16 to 16
- out_weight: bfloat16 [2048, 2048], P('heads'), may hold values from -0.125 to 0.125
Outputs:
- mixed: bfloat16 [16384, 2048], P('frames', 'heads')
- query_grad: bfloat16 [16384, 2048], P('frames', 'heads')
- key_grad: bfloat16 [16384, 2048], P('frames', 'heads')
- value_grad: bfloat16 [16384, 2048], P('frames', 'heads')
- weight_grad: bfloat16 [2048, 2048], P('heads', 'frames')
The draws below stay inside these ranges and needn't reach their ends.
All inputs are finite; a program needn't handle non-finite values.
Results may differ from the reference program's by a relative error of at most 0.014.
Values may be sent and summed in bfloat16 or wider, within the bound.
A program may use at most 64 MiB of HBM per device.

```python
import jax
import jax.numpy as jnp
from jax import lax

D = 2048
HEADS = 16
HEAD_DIM = 128
REGIONS = 128
WIN = 8
FR_DEV = 2
FRAMES = 128
TOKENS = 16384
N_FRAMES = 64
N_HEADS = 8


def paired_rows(key):
    base_queries = 2.0 * jax.random.truncated_normal(jax.random.fold_in(key, 101), -4.0, 4.0, (TOKENS, D), jnp.float32)
    base_keys = 2.0 * jax.random.truncated_normal(jax.random.fold_in(key, 102), -4.0, 4.0, (TOKENS, D), jnp.float32)
    return (base_queries, base_keys)


def draw_queries(key, part):
    return paired_rows(key)[0].astype(jnp.bfloat16)


def draw_keys(key, part):
    return paired_rows(key)[1].astype(jnp.bfloat16)


def strengthened(array, rng, source, target, blocks, factor):
    owner, partner = [(jnp.arange(array.shape[position]) // (array.shape[position] // blocks)).reshape([-1 if axis == position else 1 for axis in range(array.ndim)]) for position in (source, target)]
    chosen = jax.random.permutation(rng, blocks)[partner]
    strong = (owner == chosen) | (owner == (partner + blocks // 2) % blocks)
    return jnp.where(strong, factor * array, array)


def steps_of(rng, extent, cuts, low, largest):
    def one(position, parts):
        heights = jax.random.uniform(jax.random.fold_in(jax.random.fold_in(rng, 6), position), (parts,), jnp.float32, low / len(cuts), largest / len(cuts))
        return jnp.repeat(jnp.exp(heights), extent[position] // parts).reshape((-1,) + (1,) * (len(extent) - position - 1))

    loudness = one(*cuts[0])
    for cut in cuts[1:]:
        loudness = loudness * one(*cut)
    return loudness


def noise(stream_key, dims, spread, reach, shards=(), kind=jnp.bfloat16):
    array = jax.random.normal(stream_key, dims, jnp.float32) * spread
    if len(shards) > 0:
        array = steps_of(stream_key, dims, shards, -0.22, 0.18) * array
    return jnp.clip(array, min=-reach, max=reach).astype(kind)


def bell_draw_with(rng, shape, scale, limit, cuts, heavy, kind=jnp.bfloat16):
    drawn = scale * jax.random.normal(rng, shape, jnp.float32)
    if cuts:
        drawn = drawn * steps_of(rng, shape, cuts, -0.22, 0.18)
    return jnp.clip(strengthened(drawn, jax.random.fold_in(rng, 3), *heavy), -limit, limit).astype(kind)


def setup_inputs(seed: int = 0) -> dict:
    key_of = jax.random.split(jax.random.key(seed), 6)
    return {
        "queries": draw_queries(jax.random.fold_in(key_of[5], 71), 0),
        "keys": draw_keys(jax.random.fold_in(key_of[5], 71), 0),
        "values": noise(key_of[2], (TOKENS, D), 1.0, 6.0, ((0, 64), (1, 8))),
        "out_grad": bell_draw_with(key_of[3], (TOKENS, D), 1.0, 16.0, ((0, 64), (1, 8)), (0, 1, 64, 4.0)),
        "out_weight": noise(key_of[4], (D, D), D ** -0.5, 0.125, ((0, 8),)),
    }


def rounded(value):
    return lax.optimization_barrier(value.astype(jnp.bfloat16)).astype(jnp.float32)


def reference(queries, keys, values, out_grad, out_weight):
    block = FR_DEV * REGIONS
    margin = WIN * REGIONS
    span = block + 2 * margin
    scale = HEAD_DIM ** -0.5
    group = HEADS // N_HEADS
    padded_keys = jnp.pad(keys, ((margin, margin), (0, 0)))
    padded_values = jnp.pad(values, ((margin, margin), (0, 0)))
    weight_rows = out_weight.astype(jnp.float32).reshape(N_HEADS, group * HEAD_DIM, D)

    def advance(carry, index):
        key_acc, value_acc, weight_acc = carry
        start = index * block
        query_block = lax.dynamic_slice_in_dim(queries, start, block, 0)
        key_block = lax.dynamic_slice_in_dim(padded_keys, start, span, 0)
        value_block = lax.dynamic_slice_in_dim(padded_values, start, span, 0)
        grad_block = lax.dynamic_slice_in_dim(out_grad, start, block, 0)
        query_frame = index * FR_DEV + jnp.arange(block, dtype=jnp.int32) // REGIONS
        key_frame = index * FR_DEV - WIN + jnp.arange(span, dtype=jnp.int32) // REGIONS
        near = (jnp.abs(query_frame[:, None] - key_frame[None, :]) <= WIN) & (key_frame >= 0)[None, :] & (key_frame < FRAMES)[None, :]
        query_heads = query_block.astype(jnp.float32).reshape(block, HEADS, HEAD_DIM)
        key_heads = key_block.astype(jnp.float32).reshape(span, HEADS, HEAD_DIM)
        value_heads = value_block.astype(jnp.float32).reshape(span, HEADS, HEAD_DIM)
        scores = jnp.einsum("qhd,khd->hqk", query_heads, key_heads) * scale
        scores = jnp.where(near[None], scores, -jnp.inf)
        top = jnp.max(scores, axis=-1, keepdims=True)
        expo = jnp.where(near[None], jnp.exp(scores - top), 0.0)
        probs = expo / jnp.sum(expo, axis=-1, keepdims=True)
        weights = rounded(probs)
        attn = jnp.einsum("hqk,khd->qhd", weights, value_heads).reshape(block, D).astype(jnp.bfloat16)
        pieces = jnp.einsum("tgc,gcd->gtd", attn.astype(jnp.float32).reshape(block, N_HEADS, group * HEAD_DIM), weight_rows)
        mixed = jnp.sum(rounded(pieces), axis=0).astype(jnp.bfloat16)
        grad_attn = jnp.dot(grad_block, out_weight.T, preferred_element_type=jnp.float32).astype(jnp.bfloat16)
        grad_heads = grad_attn.astype(jnp.float32).reshape(block, HEADS, HEAD_DIM)
        dprob = jnp.einsum("qhd,khd->hqk", grad_heads, value_heads)
        delta = jnp.sum(probs * dprob, axis=-1, keepdims=True)
        dscore = rounded(probs * (dprob - delta) * scale)
        query_grad = jnp.einsum("hqk,khd->qhd", dscore, key_heads).reshape(block, D).astype(jnp.bfloat16)
        key_part = jnp.einsum("hqk,qhd->khd", dscore, query_heads).reshape(span, D)
        value_part = jnp.einsum("hqk,qhd->khd", weights, grad_heads).reshape(span, D)
        key_acc = lax.dynamic_update_slice_in_dim(key_acc, lax.dynamic_slice_in_dim(key_acc, start, span, 0) + key_part, start, 0)
        value_acc = lax.dynamic_update_slice_in_dim(value_acc, lax.dynamic_slice_in_dim(value_acc, start, span, 0) + value_part, start, 0)
        weight_acc = weight_acc + jnp.dot(attn.T, grad_block, preferred_element_type=jnp.float32)
        return (key_acc, value_acc, weight_acc), (mixed, query_grad)

    start_acc = jnp.zeros((TOKENS + 2 * margin, D), jnp.float32)
    carry = (start_acc, start_acc, jnp.zeros((D, D), jnp.float32))
    carry, (mixed, query_grad) = lax.scan(advance, carry, jnp.arange(N_FRAMES, dtype=jnp.int32))
    key_acc, value_acc, weight_acc = carry
    key_grad = key_acc[margin:margin + TOKENS].astype(jnp.bfloat16)
    value_grad = value_acc[margin:margin + TOKENS].astype(jnp.bfloat16)
    return (mixed.reshape(TOKENS, D), query_grad.reshape(TOKENS, D), key_grad, value_grad, weight_acc.astype(jnp.bfloat16))
```

```python
import jax
import jax.numpy as jnp
from jax import lax
from jax.experimental import pallas as pl
from jax.experimental.pallas import tpu as pltpu
from jax.sharding import PartitionSpec as P

MESH = pl.DeviceIdType.MESH
BF = jnp.bfloat16
F32 = jnp.float32

NZ = 8
NY = 4
NX = 4
CHIPS = NZ * NY
HD = 128
HALF = 256
TOK = 512
SCALE = HD ** (-0.5)
LOW = -1e30

K, V, Q, G = range(4)


def nt(a, b):
    return lax.dot_general(a, b, (((1,), (1,)), ((), ())), preferred_element_type=F32)


def nn(a, b):
    return jnp.dot(a, b, preferred_element_type=F32)


def kernel(
    q_hbm, k_hbm, v_hbm, og_hbm, w_hbm,
    mixed_out, dq_out, dk_out, dv_out, dw_out,
    k_in, v_in, q_in, g_in, w_in,
    buf, og_mine, og_pair, stat, scores,
    m_ref, l_ref, acc, attn_pair, attn_t, attn_tok, attn_own,
    dq_acc, dk_acc, dv_acc, stage,
    mix_send, mix_recv, mix_keep, mix_tail, mix_land,
    dw_send, dw_recv, dw_part, dw_land,
    load_sem, send_sem, tree_sem, core_sem, og_sem, ogp_sem, stat_sem,
    mix_sem, dwz_sem, dwy_sem, out_sem,
):
    f = lax.axis_index("frames")
    h = lax.axis_index("heads")
    chip = lax.div(f, 2)
    core = lax.rem(f, 2)
    other = 1 - core
    z = lax.div(chip, NY)
    y = lax.rem(chip, NY)
    ylo = lax.div(h, NX)
    x = lax.rem(h, NX)

    def at(c, k):
        return (c * 2 + k, h)

    def along_x(step):
        return (f, ylo * NX + lax.rem(x + step + NX, NX))

    pair = (f + 1 - 2 * core, h)
    across = (f, (1 - ylo) * NX + x)
    mine = pl.ds(pl.multiple_of(core * HALF, HALF), HALF)
    theirs = pl.ds(pl.multiple_of(other * HALF, HALF), HALF)
    my_head = pl.ds(pl.multiple_of(core * HD, HD), HD)
    their_head = pl.ds(pl.multiple_of(other * HD, HD), HD)

    loads = []
    for i, (src, dst) in enumerate((
        (k_hbm, k_in), (v_hbm, v_in), (og_hbm, og_mine.at[h]), (q_hbm, q_in), (w_hbm, w_in),
    )):
        copy = pltpu.make_async_copy(src, dst, load_sem.at[i])
        copy.start()
        loads.append(copy)

    barrier = pltpu.get_barrier_semaphore()
    peers = [pair, across, along_x(1), along_x(2), along_x(3)]
    for step in (1, CHIPS - 1):
        for k in range(2):
            peers.append(at(lax.rem(chip + step, CHIPS), k))
    for step in (2, CHIPS - 2):
        peers.append(at(lax.rem(chip + step, CHIPS), core))
    for step in range(1, NZ):
        peers.append(at(lax.rem(chip + step * NY, CHIPS), core))
    for step in range(1, NY):
        for k in range(2):
            peers.append(at(z * NY + lax.rem(y + step, NY), k))
    for peer in peers:
        pl.semaphore_signal(barrier, inc=1, device_id=peer, device_id_type=MESH)
    pl.semaphore_wait(barrier, len(peers))

    sent = []

    def when(cond, fn):
        if cond is None:
            fn()
        else:
            pl.when(cond)(fn)

    def send(src, dst, sem, device, cond=None):
        slot = len(sent)

        def make():
            return pltpu.make_async_remote_copy(
                src_ref=src, dst_ref=dst, send_sem=send_sem.at[slot], recv_sem=sem,
                device_id=device, device_id_type=MESH,
            )

        sent.append((make, cond))
        when(cond, lambda: make().start())

    def recv(dst, sem, cond=None):
        when(cond, lambda: pltpu.make_async_remote_copy(
            src_ref=dst, dst_ref=dst, send_sem=send_sem.at[0], recv_sem=sem,
            device_id=pair, device_id_type=MESH,
        ).wait_recv())

    def rows(j):
        return pl.ds(j * HALF, HALF)

    def spread(t, src):
        for step, slot in ((1, 1), (-1, 3)):
            cond = chip < CHIPS - 1 if step > 0 else chip > 0
            for k in range(2):
                send(src.at[:, pl.ds(k * HD, HD)], buf.at[t, slot, mine], tree_sem.at[t, slot, core],
                     at(chip + step, k), cond)

    def chunk(t, slot, j):
        return buf.at[t, slot, rows(j)], tree_sem.at[t, slot, j]

    def arrive(t, slot, j, cond):
        recv(*chunk(t, slot, j), cond)

    def pass_on(t, slot, j, to_slot, step, cond):
        dst, sem = chunk(t, to_slot, j)
        send(buf.at[t, slot, rows(j)], dst, sem, at(chip + step, core), cond)

    has_left, has_right = chip >= 1, chip <= CHIPS - 2
    inner = has_left & has_right

    def relay_near(t):
        arrive(t, 1, 0, has_left)
        pass_on(t, 1, 0, 0, 1, inner)
        arrive(t, 3, 1, has_right)
        pass_on(t, 3, 1, 4, -1, inner)
        arrive(t, 1, 1, has_left)
        pass_on(t, 1, 1, 0, 1, has_left & (chip <= 2))
        arrive(t, 3, 0, has_right)
        pass_on(t, 3, 0, 4, -1, has_right & (chip >= CHIPS - 3))

    def relay_far(t):
        arrive(t, 0, 0, chip >= 2)
        pass_on(t, 0, 0, 4, -NY, chip >= NY)
        arrive(t, 4, 1, chip <= CHIPS - 3)
        pass_on(t, 4, 1, 0, NY, chip <= CHIPS - 1 - NY)

    def relay_last(t):
        arrive(t, 0, 1, chip >= 2)
        arrive(t, 4, 0, chip <= CHIPS - 3)

    def live(slot):
        block = chip + slot - 2
        return (block >= 0) & (block < CHIPS)

    loads[0].wait()
    send(k_in.at[:, their_head], buf.at[K, 2, mine], core_sem.at[K], pair)
    spread(K, k_in)
    loads[2].wait()
    send(og_mine.at[h], og_mine.at[h], og_sem.at[h], across)
    send(og_mine.at[h], og_mine.at[h], og_sem.at[h], along_x(1))
    send(og_mine.at[h], og_mine.at[h], og_sem.at[h], along_x(-1))
    loads[1].wait()
    send(v_in.at[:, their_head], buf.at[V, 2, mine], core_sem.at[V], pair)
    spread(V, v_in)
    loads[3].wait()
    send(q_in.at[:, their_head], buf.at[Q, 2, mine], core_sem.at[Q], pair)
    send(og_mine.at[h], og_pair.at[h], ogp_sem.at[h], pair)
    buf[K, 2, mine] = k_in[:, my_head]
    buf[V, 2, mine] = v_in[:, my_head]
    buf[Q, 2, mine] = q_in[:, my_head]
    m_ref[...] = jnp.full_like(m_ref, LOW)
    l_ref[...] = jnp.zeros_like(l_ref)
    acc[...] = jnp.zeros_like(acc)
    dq_acc[...] = jnp.zeros_like(dq_acc)
    dk_acc[...] = jnp.zeros_like(dk_acc)
    dv_acc[...] = jnp.zeros_like(dv_acc)

    def og_take(b):
        recv(og_mine.at[b], og_sem.at[b])
        send(og_mine.at[b], og_pair.at[b], ogp_sem.at[b], pair)

    def og_on(b, step):
        send(og_mine.at[b], og_mine.at[b], og_sem.at[b], along_x(step))

    def block_of(row, step):
        return row * NX + lax.rem(x + step + NX, NX)

    b = block_of(1 - ylo, 0)
    og_take(b)
    og_on(b, 1)
    og_on(b, -1)

    def near_mask(slot, key_frame, query_frame, shape):
        keys = lax.broadcasted_iota(jnp.int32, shape, 0) // HD + key_frame
        queries = lax.broadcasted_iota(jnp.int32, shape, 1) // HD + query_frame
        gap = (keys - queries) * jnp.where(slot == 0, 1, -1)
        return gap >= 0

    def attend(slot, j, masked):
        idx = slot * 2 + j
        keys = buf[K, slot, pl.ds(pl.multiple_of(j * HALF, HALF), HALF)]
        vals_t = buf[V, slot, pl.ds(pl.multiple_of(j * HALF, HALF), HALF)].T
        for part in range(2):
            lanes = pl.ds(part * HALF, HALF)
            s = nt(keys, buf[Q, 2, lanes]) * SCALE
            if masked:
                s = jnp.where(near_mask(slot, 2 * j, 2 * part, s.shape), s, LOW)
            scores[idx, :, lanes] = s
            old = m_ref[:, lanes]
            new = jnp.maximum(old, jnp.max(s, axis=0, keepdims=True))
            p = jnp.exp(s - new)
            fade = jnp.exp(old - new)
            m_ref[:, lanes] = new
            l_ref[:, lanes] = l_ref[:, lanes] * fade + jnp.sum(p, axis=0, keepdims=True)
            acc[:, lanes] = acc[:, lanes] * fade + nn(vals_t, p.astype(BF))

    def attend_all(pairs, masked):
        def step(i, carry):
            slot, j = pairs(i)
            pl.when(live(slot))(lambda: attend(slot, j, masked))
            return carry
        return step

    recv(buf.at[K, 2, theirs], core_sem.at[K])
    recv(buf.at[V, 2, theirs], core_sem.at[V])
    recv(buf.at[Q, 2, theirs], core_sem.at[Q])
    lax.fori_loop(0, 2, attend_all(lambda i: (2, i), False), 0)

    b = block_of(ylo, -1)
    og_take(b)
    og_on(b, 1)
    b = block_of(1 - ylo, 1)
    og_take(b)
    og_on(b, -1)
    og_take(block_of(ylo, 1))
    og_take(block_of(1 - ylo, -1))

    relay_near(K)
    relay_near(V)
    spread(Q, q_in)

    og_take(block_of(ylo, 2))
    og_take(block_of(1 - ylo, 2))
    loads[4].wait()

    grad = jnp.zeros((HALF, HALF), F32)

    def grad_step(i, total):
        cols = pl.ds(pl.multiple_of(i * HALF, HALF), HALF)
        return total + nt(og_mine[i], w_in[:, cols])

    g_in[...] = lax.fori_loop(0, 8, grad_step, grad).astype(BF)
    buf[G, 2, mine] = g_in[:, my_head]
    send(g_in.at[:, their_head], buf.at[G, 2, mine], core_sem.at[G], pair)

    lax.fori_loop(0, 4, attend_all(lambda i: (1 + 2 * lax.rem(i, 2), lax.div(i, 2)), False), 0)

    relay_far(K)
    relay_far(V)
    relay_near(Q)
    spread(G, g_in)
    lax.fori_loop(0, 2, attend_all(lambda i: (4 * i, i), True), 0)
    relay_last(K)
    relay_last(V)
    lax.fori_loop(0, 2, attend_all(lambda i: (4 * i, 1 - i), True), 0)
    recv(buf.at[G, 2, theirs], core_sem.at[G])

    total = l_ref[...]
    out = acc[...] / total
    lse = m_ref[...] + jnp.log(total)
    g_t = buf[G, 2].astype(F32).T
    delta = jnp.sum(g_t * out, axis=0, keepdims=True)
    for i in range(4):
        stat[2, i:i + 1] = lse[:, i * HD:(i + 1) * HD]
        stat[2, 4 + i:5 + i] = delta[:, i * HD:(i + 1) * HD]
    m_ref[...] = lse
    l_ref[...] = delta
    attn_t[...] = out.astype(BF)
    attn_tok[...] = out.T.astype(BF)
    send(attn_tok.at[theirs], attn_own.at[:, my_head], core_sem.at[4], pair)
    attn_own[:, my_head] = attn_tok[mine]
    for step in (1, -1, 2, -2):
        cond = chip + step < CHIPS if step > 0 else chip + step >= 0
        send(stat.at[2], stat.at[2 - step], stat_sem.at[2 - step], at(chip + step, core), cond)

    for b in range(8):
        recv(og_pair.at[b], ogp_sem.at[b])

    def dw_step(i, carry):
        plane = lax.rem(z + i, NZ)
        part = nn(attn_t[:, mine], og_mine[plane]) + nn(attn_t[:, theirs], og_pair[plane])
        dw_send[i] = part.astype(BF)
        return carry

    lax.fori_loop(0, NZ, dw_step, 0)
    for i in (4, 3, 5, 2, 6, 1, 7):
        send(dw_send.at[i], dw_recv.at[i], dwz_sem.at[i], at(lax.rem(z + i, NZ) * NY + y, core))

    recv(attn_own.at[:, their_head], core_sem.at[4])
    for step in (2, 1, 3, 0):
        def mix_step(i, carry):
            cols = pl.ds(pl.multiple_of((i * NX + lax.rem(x + step, NX)) * HALF, HALF), HALF)
            part = nn(attn_own[...], w_in[:, cols])
            if step:
                mix_send[step - 1, i] = part.astype(BF)
            else:
                mix_keep[i] = part
            return carry
        lax.fori_loop(0, 2, mix_step, 0)
        if step:
            send(mix_send.at[step - 1], mix_recv.at[step - 1], mix_sem.at[step - 1], along_x(step))

    relay_far(Q)
    relay_near(G)

    def query_grad(i, carry):
        slot, j = lax.div(i, 2), lax.rem(i, 2)

        def run():
            at_rows = pl.ds(pl.multiple_of(j * HALF, HALF), HALF)
            keys_t = buf[K, slot, at_rows].T
            vals = buf[V, slot, at_rows]
            for part in range(2):
                lanes = pl.ds(part * HALF, HALF)
                p = jnp.exp(scores[i, :, lanes] - m_ref[:, lanes])
                d = nt(vals, buf[G, 2, lanes])
                ds = (p * (d - l_ref[:, lanes]) * SCALE).astype(BF)
                dq_acc[:, lanes] += nn(keys_t, ds)

        pl.when(live(slot))(run)
        return carry

    lax.fori_loop(0, 10, query_grad, 0)
    stage[0] = dq_acc[...].T.astype(BF)
    send(stage.at[0, theirs], dq_out.at[:, my_head], out_sem.at[0], pair)
    dq_out[:, my_head] = stage[0, mine]

    def collect(slot, j, masked):
        at_rows = pl.ds(pl.multiple_of(j * HALF, HALF), HALF)
        qs = buf[Q, slot, at_rows]
        gs = buf[G, slot, at_rows]

        def row(first):
            return jnp.concatenate(
                [stat[slot, pl.ds(first + 2 * j, 1)], stat[slot, pl.ds(first + 2 * j + 1, 1)]], axis=1)

        lse_row, delta_row = row(0), row(4)
        for part in range(2):
            own = pl.ds(part * HALF, HALF)
            s = nt(buf[K, 2, own], qs) * SCALE
            p = jnp.exp(s - lse_row)
            if masked:
                p = jnp.where(near_mask(4 - slot, 2 * part, 2 * j, p.shape), p, 0.0)
            d = nt(buf[V, 2, own], gs)
            ds = (p * (d - delta_row) * SCALE).astype(BF)
            dv_acc[own] += nn(p.astype(BF), gs)
            dk_acc[own] += nn(ds, qs)

    def collect_all(pairs, masked):
        def step(i, carry):
            slot, j = pairs(i)
            pl.when(live(slot))(lambda: collect(slot, j, masked))
            return carry
        return step

    lax.fori_loop(0, 2, collect_all(lambda i: (2, i), False), 0)
    relay_last(Q)

    for step in (1, 2, 3):
        recv(mix_recv.at[step - 1], mix_sem.at[step - 1])

    def mix_sum(i):
        return mix_keep[i] + sum(mix_recv[s, i].astype(F32) for s in range(3))

    mix_tail[...] = mix_sum(1 - ylo).astype(BF)
    send(mix_tail, mix_land, mix_sem.at[3], across)

    for i in (1, 7, 2, 6, 3, 5, 4):
        recv(dw_recv.at[i], dwz_sem.at[i])
    part = dw_send[0].astype(F32)
    for i in range(1, NZ):
        part = part + dw_recv[i].astype(F32)
    dw_part[...] = part.T.astype(BF)

    def cut(yy, k):
        return pl.ds(pl.multiple_of((yy * 2 + k) * 32, 32), 32)

    for step in range(NY):
        yy = lax.rem(y + step, NY)
        for far in range(2):
            k = core if far == 0 else other
            if step == 0 and far == 0:
                dw_land[0, core] = dw_part[cut(yy, k)]
            else:
                send(dw_part.at[cut(yy, k)], dw_land.at[step, core], dwy_sem.at[step, core],
                     at(z * NY + yy, k))

    for i in range(4):
        slot = (1, 3, 0, 4)[i]
        recv(stat.at[slot], stat_sem.at[slot], live(slot))
    relay_far(G)
    lax.fori_loop(0, 4, collect_all(lambda i: (1 + 2 * lax.rem(i, 2), lax.div(i, 2)), False), 0)
    lax.fori_loop(0, 2, collect_all(lambda i: (4 * i, i), True), 0)
    recv(mix_land, mix_sem.at[3])
    mixed_out[...] = (mix_sum(ylo) + mix_land[...].astype(F32)).astype(BF)
    for step in range(NY):
        for far in range(2):
            k = core if far == 0 else other
            if not (step == 0 and far == 0):
                recv(dw_land.at[step, k], dwy_sem.at[step, k])
    for k in range(2):
        piece = sum(dw_land[s, k].astype(F32) for s in range(NY))
        dw_out[k * HD:(k + 1) * HD] = piece.T.astype(BF)
    relay_last(G)
    lax.fori_loop(0, 2, collect_all(lambda i: (4 * i, 1 - i), True), 0)
    for i, (total_ref, out_ref) in enumerate(((dk_acc, dk_out), (dv_acc, dv_out))):
        stage[1 + i] = total_ref[...].astype(BF)
        send(stage.at[1 + i, theirs], out_ref.at[:, my_head], out_sem.at[1 + i], pair)
        out_ref[:, my_head] = stage[1 + i, mine]
    for i, out_ref in enumerate((dq_out, dk_out, dv_out)):
        recv(out_ref.at[:, their_head], out_sem.at[i])
    for make, cond in sent:
        when(cond, lambda: make().wait_send())


SENDS = 128


def body(queries, keys, values, out_grad, out_weight):
    block = jax.ShapeDtypeStruct((HALF, HALF), BF)
    dma = pltpu.SemaphoreType.DMA
    vmem = pltpu.VMEM
    return pl.pallas_call(
        kernel,
        out_shape=(block, block, block, block, jax.ShapeDtypeStruct((HALF, 32), BF)),
        in_specs=[pl.BlockSpec(memory_space=pltpu.HBM)] * 5,
        out_specs=[pl.BlockSpec(memory_space=pltpu.VMEM)] * 5,
        scratch_shapes=[
            vmem((HALF, HALF), BF),
            vmem((HALF, HALF), BF),
            vmem((HALF, HALF), BF),
            vmem((HALF, HALF), BF),
            vmem((HALF, 2048), BF),
            vmem((4, 5, TOK, HD), BF),
            vmem((8, HALF, HALF), BF),
            vmem((8, HALF, HALF), BF),
            vmem((5, 8, HD), F32),
            vmem((10, HALF, TOK), F32),
            vmem((1, TOK), F32),
            vmem((1, TOK), F32),
            vmem((HD, TOK), F32),
            vmem((8, HD), F32),
            vmem((HD, TOK), BF),
            vmem((TOK, HD), BF),
            vmem((HALF, HALF), BF),
            vmem((HD, TOK), F32),
            vmem((TOK, HD), F32),
            vmem((TOK, HD), F32),
            vmem((3, TOK, HD), BF),
            vmem((3, 2, HALF, HALF), BF),
            vmem((3, 2, HALF, HALF), BF),
            vmem((2, HALF, HALF), F32),
            vmem((HALF, HALF), BF),
            vmem((HALF, HALF), BF),
            vmem((NZ, HD, HALF), BF),
            vmem((NZ, HD, HALF), BF),
            vmem((HALF, HD), BF),
            vmem((NY, 2, 32, HD), BF),
            dma((5,)),
            dma((SENDS,)),
            dma((4, 5, 2)),
            dma((5,)),
            dma((8,)),
            dma((8,)),
            dma((5,)),
            dma((4,)),
            dma((NZ,)),
            dma((NY, 2)),
            dma((3,)),
        ],
        compiler_params=pltpu.CompilerParams(
            collective_id=0, has_side_effects=True, vmem_limit_bytes=60 * 2**20
        ),
    )(queries, keys, values, out_grad, out_weight)


def solution(mesh):
    placed = (
        P("frames", "heads"),
        P("frames", "heads"),
        P("frames", "heads"),
        P("frames", "heads"),
        P("heads", None),
    )
    return jax.shard_map(
        body,
        mesh=mesh,
        in_specs=placed,
        out_specs=(
            P("frames", "heads"),
            P("frames", "heads"),
            P("frames", "heads"),
            P("frames", "heads"),
            P("heads", "frames"),
        ),
        check_vma=False,
    )
```

```python
import jax
import jax.numpy as jnp
from jax import lax
from jax.experimental import pallas as pl
from jax.experimental.pallas import tpu as pltpu
from jax.sharding import PartitionSpec as P

MESH = pl.DeviceIdType.MESH
BF = jnp.bfloat16
F32 = jnp.float32

NZ = 8
NY = 4
NX = 4
CHIPS = NZ * NY
HD = 128
HALF = 256
TOK = 512
SCALE = HD ** (-0.5)
LOW = -1e30

K, V, Q, G = range(4)


def nt(a, b):
    return lax.dot_general(a, b, (((1,), (1,)), ((), ())), preferred_element_type=F32)


def nn(a, b):
    return jnp.dot(a, b, preferred_element_type=F32)


def kernel(
    q_hbm, k_hbm, v_hbm, og_hbm, w_hbm,
    mixed_out, dq_out, dk_out, dv_out, dw_out,
    k_in, v_in, q_in, g_in, w_in,
    buf, og_mine, og_pair, stat, scores,
    m_ref, l_ref, acc, attn_t, attn_tok, attn_own,
    dq_acc, dk_acc, dv_acc, stage,
    mix_send, mix_recv, mix_keep, mix_tail, mix_land,
    dw_send, dw_recv, dw_part, dw_land,
    load_sem, send_sem, tree_sem, core_sem, og_sem, ogp_sem, stat_sem,
    mix_sem, dwz_sem, dwy_sem, out_sem, plane_sem,
):
    f = lax.axis_index("frames")
    h = lax.axis_index("heads")
    chip = lax.div(f, 2)
    core = lax.rem(f, 2)
    other = 1 - core
    z = lax.div(chip, NY)
    y = lax.rem(chip, NY)
    ylo = lax.div(h, NX)
    x = lax.rem(h, NX)

    def at(c, k):
        return (c * 2 + k, h)

    def along_x(step):
        return (f, ylo * NX + lax.rem(x + step + NX, NX))

    pair = (f + 1 - 2 * core, h)
    across = (f, (1 - ylo) * NX + x)
    mine = pl.ds(pl.multiple_of(core * HALF, HALF), HALF)
    theirs = pl.ds(pl.multiple_of(other * HALF, HALF), HALF)
    my_head = pl.ds(pl.multiple_of(core * HD, HD), HD)
    their_head = pl.ds(pl.multiple_of(other * HD, HD), HD)

    loads = []
    for i, (src, dst) in enumerate((
        (og_hbm, og_mine.at[h]), (k_hbm, k_in), (v_hbm, v_in), (q_hbm, q_in), (w_hbm, w_in),
    )):
        copy = pltpu.make_async_copy(src, dst, load_sem.at[i])
        copy.start()
        loads.append(copy)

    barrier = pltpu.get_barrier_semaphore()

    def in_reach(step):
        return (chip + step >= 0) & (chip + step < CHIPS)

    def greet(device):
        pl.semaphore_signal(barrier, inc=1, device_id=device, device_id_type=MESH)

    peers = [pair, across, along_x(1), along_x(2), along_x(3)]
    for step in range(1, NY):
        for k in range(2):
            peers.append(at(z * NY + lax.rem(y + step, NY), k))
    for peer in peers:
        greet(peer)
    expected = len(peers)
    for step in (1, -1, 2, -2, NY, -NY):
        def greet_chip(step=step):
            for k in (0, 1) if abs(step) == 1 else (core,):
                greet(at(chip + step, k))

        pl.when(in_reach(step))(greet_chip)
        expected = expected + jnp.where(in_reach(step), 2 if abs(step) == 1 else 1, 0)
    pl.semaphore_wait(barrier, expected)

    def tell(way, step, cond):
        pl.when(cond)(lambda: pl.semaphore_signal(
            plane_sem.at[way], inc=1, device_id=at(chip + step, core), device_id_type=MESH))

    tell(0, NY, z == 0)
    tell(1, -NY, z == NZ - 1)

    def hear_planes(i):
        @pl.when(z == i + 1)
        def _():
            pl.semaphore_wait(plane_sem.at[0], 1)

        tell(0, NY, (z == i + 1) & (z < NZ - 1))

        @pl.when(z == NZ - 2 - i)
        def _():
            pl.semaphore_wait(plane_sem.at[1], 1)

        tell(1, -NY, (z == NZ - 2 - i) & (z > 0))

    sent = []

    def when(cond, fn):
        if cond is None:
            fn()
        else:
            pl.when(cond)(fn)

    def send(src, dst, sem, device, cond=None):
        slot = len(sent)

        def make():
            return pltpu.make_async_remote_copy(
                src_ref=src, dst_ref=dst, send_sem=send_sem.at[slot], recv_sem=sem,
                device_id=device, device_id_type=MESH,
            )

        sent.append((make, cond))
        when(cond, lambda: make().start())

    def recv(dst, sem, cond=None):
        when(cond, lambda: pltpu.make_async_remote_copy(
            src_ref=dst, dst_ref=dst, send_sem=send_sem.at[0], recv_sem=sem,
            device_id=pair, device_id_type=MESH,
        ).wait_recv())

    def rows(j):
        return pl.ds(j * HALF, HALF)

    def spread(t, src):
        for step, slot in ((1, 1), (-1, 3)):
            cond = chip < CHIPS - 1 if step > 0 else chip > 0
            for k in range(2):
                send(src.at[:, pl.ds(k * HD, HD)], buf.at[t, slot, mine], tree_sem.at[t, slot, core],
                     at(chip + step, k), cond)

    def chunk(t, slot, j):
        return buf.at[t, slot, rows(j)], tree_sem.at[t, slot, j]

    def arrive(t, slot, j, cond):
        recv(*chunk(t, slot, j), cond)

    def pass_on(t, slot, j, to_slot, step, cond):
        dst, sem = chunk(t, to_slot, j)
        send(buf.at[t, slot, rows(j)], dst, sem, at(chip + step, core), cond)

    has_left, has_right = chip >= 1, chip <= CHIPS - 2
    inner = has_left & has_right

    def relay_near(t):
        arrive(t, 1, 0, has_left)
        pass_on(t, 1, 0, 0, 1, inner)
        arrive(t, 3, 1, has_right)
        pass_on(t, 3, 1, 4, -1, inner)
        arrive(t, 1, 1, has_left)
        pass_on(t, 1, 1, 0, 1, has_left & (chip <= 2))
        arrive(t, 3, 0, has_right)
        pass_on(t, 3, 0, 4, -1, has_right & (chip >= CHIPS - 3))

    def relay_far(t):
        arrive(t, 0, 0, chip >= 2)
        pass_on(t, 0, 0, 4, -NY, chip >= NY)
        arrive(t, 4, 1, chip <= CHIPS - 3)
        pass_on(t, 4, 1, 0, NY, chip <= CHIPS - 1 - NY)

    def relay_last(t):
        arrive(t, 0, 1, chip >= 2)
        arrive(t, 4, 0, chip <= CHIPS - 3)

    def live(slot):
        block = chip + slot - 2
        return (block >= 0) & (block < CHIPS)

    loads[0].wait()
    send(og_mine.at[h], og_mine.at[h], og_sem.at[h], across)
    send(og_mine.at[h], og_mine.at[h], og_sem.at[h], along_x(1))
    send(og_mine.at[h], og_mine.at[h], og_sem.at[h], along_x(-1))
    loads[1].wait()
    send(k_in.at[:, their_head], buf.at[K, 2, mine], core_sem.at[K], pair)
    spread(K, k_in)
    loads[2].wait()
    send(v_in.at[:, their_head], buf.at[V, 2, mine], core_sem.at[V], pair)
    loads[3].wait()
    send(q_in.at[:, their_head], buf.at[Q, 2, mine], core_sem.at[Q], pair)
    spread(V, v_in)
    send(og_mine.at[h], og_pair.at[h], ogp_sem.at[h], pair)
    buf[K, 2, mine] = k_in[:, my_head]
    buf[V, 2, mine] = v_in[:, my_head]
    buf[Q, 2, mine] = q_in[:, my_head]
    m_ref[...] = jnp.full_like(m_ref, LOW)
    l_ref[...] = jnp.zeros_like(l_ref)
    acc[...] = jnp.zeros_like(acc)
    dq_acc[...] = jnp.zeros_like(dq_acc)
    dk_acc[...] = jnp.zeros_like(dk_acc)
    dv_acc[...] = jnp.zeros_like(dv_acc)

    def og_take(b):
        recv(og_mine.at[b], og_sem.at[b])
        send(og_mine.at[b], og_pair.at[b], ogp_sem.at[b], pair)

    def og_on(b, step):
        send(og_mine.at[b], og_mine.at[b], og_sem.at[b], along_x(step))

    def block_of(row, step):
        return row * NX + lax.rem(x + step + NX, NX)

    def near_mask(slot, key_frame, query_frame, shape):
        keys = lax.broadcasted_iota(jnp.int32, shape, 0) // HD + key_frame
        queries = lax.broadcasted_iota(jnp.int32, shape, 1) // HD + query_frame
        gap = (keys - queries) * jnp.where(slot == 0, 1, -1)
        return gap >= 0

    def attend(slot, j, masked):
        idx = slot * 2 + j
        keys = buf[K, slot, pl.ds(pl.multiple_of(j * HALF, HALF), HALF)]
        vals_t = buf[V, slot, pl.ds(pl.multiple_of(j * HALF, HALF), HALF)].T
        for part in range(2):
            lanes = pl.ds(part * HALF, HALF)
            s = nt(keys, buf[Q, 2, lanes]) * SCALE
            if masked:
                s = jnp.where(near_mask(slot, 2 * j, 2 * part, s.shape), s, LOW)
            scores[idx, :, lanes] = s
            old = m_ref[:, lanes]
            new = jnp.maximum(old, jnp.max(s, axis=0, keepdims=True))
            p = jnp.exp(s - new)
            fade = jnp.exp(old - new)
            m_ref[:, lanes] = new
            l_ref[:, lanes] = l_ref[:, lanes] * fade + jnp.sum(p, axis=0, keepdims=True)
            acc[:, lanes] = acc[:, lanes] * fade + nn(vals_t, p.astype(BF))

    def attend_all(pairs, masked):
        def step(i, carry):
            slot, j = pairs(i)
            pl.when(live(slot))(lambda: attend(slot, j, masked))
            return carry
        return step

    recv(buf.at[K, 2, theirs], core_sem.at[K])
    recv(buf.at[V, 2, theirs], core_sem.at[V])
    recv(buf.at[Q, 2, theirs], core_sem.at[Q])
    lax.fori_loop(0, 2, attend_all(lambda i: (2, i), False), 0)

    hear_planes(0)
    b = block_of(ylo, -1)
    og_take(b)
    og_on(b, 1)
    og_take(block_of(ylo, 1))
    b = block_of(1 - ylo, 0)
    og_take(b)
    og_on(b, 1)
    og_on(b, -1)
    hear_planes(1)
    b = block_of(1 - ylo, 1)
    og_take(b)
    og_on(b, -1)
    og_take(block_of(1 - ylo, -1))
    relay_near(K)
    hear_planes(2)
    og_take(block_of(ylo, 2))
    og_take(block_of(1 - ylo, 2))
    loads[4].wait()

    grad = jnp.zeros((HALF, HALF), F32)

    def grad_step(i, total):
        cols = pl.ds(pl.multiple_of(i * HALF, HALF), HALF)
        return total + nt(og_mine[i], w_in[:, cols])

    g_in[...] = lax.fori_loop(0, 8, grad_step, grad).astype(BF)
    buf[G, 2, mine] = g_in[:, my_head]
    send(g_in.at[:, their_head], buf.at[G, 2, mine], core_sem.at[G], pair)

    hear_planes(3)
    relay_near(V)
    spread(Q, q_in)
    hear_planes(4)
    lax.fori_loop(0, 4, attend_all(lambda i: (1 + 2 * lax.rem(i, 2), lax.div(i, 2)), False), 0)
    relay_far(K)
    hear_planes(5)
    relay_far(V)
    spread(G, g_in)
    hear_planes(6)
    lax.fori_loop(0, 2, attend_all(lambda i: (4 * i, i), True), 0)
    relay_last(K)
    relay_last(V)
    lax.fori_loop(0, 2, attend_all(lambda i: (4 * i, 1 - i), True), 0)
    recv(buf.at[G, 2, theirs], core_sem.at[G])

    total = l_ref[...]
    out = acc[...] / total
    lse = m_ref[...] + jnp.log(total)
    g_t = buf[G, 2].astype(F32).T
    delta = jnp.sum(g_t * out, axis=0, keepdims=True)
    for i in range(4):
        stat[2, i:i + 1] = lse[:, i * HD:(i + 1) * HD]
        stat[2, 4 + i:5 + i] = delta[:, i * HD:(i + 1) * HD]
    m_ref[...] = lse
    l_ref[...] = delta
    attn_t[...] = out.astype(BF)
    attn_tok[...] = out.T.astype(BF)
    send(attn_tok.at[theirs], attn_own.at[:, my_head], core_sem.at[4], pair)
    attn_own[:, my_head] = attn_tok[mine]
    for step in (1, -1, 2, -2):
        cond = chip + step < CHIPS if step > 0 else chip + step >= 0
        send(stat.at[2], stat.at[2 - step], stat_sem.at[2 - step], at(chip + step, core), cond)

    recv(attn_own.at[:, their_head], core_sem.at[4])

    def mix_part(side, step):
        row = 1 - ylo if side == 0 else ylo
        cols = pl.ds(pl.multiple_of((row * NX + lax.rem(x + step, NX)) * HALF, HALF), HALF)
        return nn(attn_own[...], w_in[:, cols])

    for side in range(2):
        def mix_step(i, carry):
            mix_send[i, side] = mix_part(side, i + 1).astype(BF)
            return carry

        lax.fori_loop(0, 3, mix_step, 0)
        for i in (1, 0, 2):
            send(mix_send.at[i, side], mix_recv.at[i, side], mix_sem.at[i, side], along_x(i + 1))
    relay_near(Q)

    for b in range(8):
        recv(og_pair.at[b], ogp_sem.at[b])

    def dw_step(plane, carry):
        part = nn(attn_t[:, mine], og_mine[plane]) + nn(attn_t[:, theirs], og_pair[plane])
        dw_send[plane] = part.astype(BF)
        return carry

    for first in (0, 4):
        lax.fori_loop(first, first + 4, dw_step, 0)
        for plane in range(first, first + 4):
            send(dw_send.at[plane], dw_recv.at[z], dwz_sem.at[z], at(plane * NY + y, core), z != plane)
    mix_keep[0] = mix_part(0, 0)
    mix_keep[1] = mix_part(1, 0)

    def query_grad(i, carry):
        slot, j = lax.div(i, 2), lax.rem(i, 2)

        def run():
            at_rows = pl.ds(pl.multiple_of(j * HALF, HALF), HALF)
            keys_t = buf[K, slot, at_rows].T
            vals = buf[V, slot, at_rows]
            for part in range(2):
                lanes = pl.ds(part * HALF, HALF)
                p = jnp.exp(scores[i, :, lanes] - m_ref[:, lanes])
                d = nt(vals, buf[G, 2, lanes])
                ds = (p * (d - l_ref[:, lanes]) * SCALE).astype(BF)
                dq_acc[:, lanes] += nn(keys_t, ds)

        pl.when(live(slot))(run)
        return carry

    def collect(slot, j, masked):
        at_rows = pl.ds(pl.multiple_of(j * HALF, HALF), HALF)
        qs = buf[Q, slot, at_rows]
        gs = buf[G, slot, at_rows]

        def row(first):
            return jnp.concatenate(
                [stat[slot, pl.ds(first + 2 * j, 1)], stat[slot, pl.ds(first + 2 * j + 1, 1)]], axis=1)

        lse_row, delta_row = row(0), row(4)
        for part in range(2):
            own = pl.ds(part * HALF, HALF)
            s = nt(buf[K, 2, own], qs) * SCALE
            p = jnp.exp(s - lse_row)
            if masked:
                p = jnp.where(near_mask(4 - slot, 2 * part, 2 * j, p.shape), p, 0.0)
            d = nt(buf[V, 2, own], gs)
            ds = (p * (d - delta_row) * SCALE).astype(BF)
            dv_acc[own] += nn(p.astype(BF), gs)
            dk_acc[own] += nn(ds, qs)

    def collect_all(pairs, masked):
        def step(i, carry):
            slot, j = pairs(i)
            pl.when(live(slot))(lambda: collect(slot, j, masked))
            return carry
        return step

    lax.fori_loop(0, 4, query_grad, 0)
    relay_near(G)
    for slot in (1, 3, 0, 4):
        recv(stat.at[slot], stat_sem.at[slot], live(slot))
    relay_far(Q)
    lax.fori_loop(4, 10, query_grad, 0)
    stage[0] = dq_acc[...].T.astype(BF)
    send(stage.at[0, theirs], dq_out.at[:, my_head], out_sem.at[0], pair)
    dq_out[:, my_head] = stage[0, mine]
    lax.fori_loop(0, 2, collect_all(lambda i: (2, i), False), 0)
    relay_far(G)

    def mix_sum(side):
        for i in range(3):
            recv(mix_recv.at[i, side], mix_sem.at[i, side])
        return mix_keep[side] + sum(mix_recv[i, side].astype(F32) for i in range(3))

    mix_tail[...] = mix_sum(0).astype(BF)
    send(mix_tail, mix_land, mix_sem.at[3, 0], across)
    lax.fori_loop(0, 4, collect_all(lambda i: (1 + 2 * lax.rem(i, 2), lax.div(i, 2)), False), 0)
    mix_keep[1] = mix_sum(1)

    dw_recv[z] = dw_send[z]
    for plane in range(NZ):
        recv(dw_recv.at[plane], dwz_sem.at[plane], z != plane)
    part = dw_recv[0].astype(F32)
    for plane in range(1, NZ):
        part = part + dw_recv[plane].astype(F32)
    dw_part[...] = part.T.astype(BF)

    def cut(yy, k):
        return pl.ds(pl.multiple_of((yy * 2 + k) * 32, 32), 32)

    for step in range(NY):
        yy = lax.rem(y + step, NY)
        for far in range(2):
            k = core if far == 0 else other
            if step == 0 and far == 0:
                dw_land[0, core] = dw_part[cut(yy, k)]
            else:
                send(dw_part.at[cut(yy, k)], dw_land.at[step, core], dwy_sem.at[step, core],
                     at(z * NY + yy, k))

    relay_last(Q)
    lax.fori_loop(0, 2, collect_all(lambda i: (4 * i, i), True), 0)
    relay_last(G)
    lax.fori_loop(0, 2, collect_all(lambda i: (4 * i, 1 - i), True), 0)
    for i, (total_ref, out_ref) in enumerate(((dk_acc, dk_out), (dv_acc, dv_out))):
        stage[1 + i] = total_ref[...].astype(BF)
        send(stage.at[1 + i, theirs], out_ref.at[:, my_head], out_sem.at[1 + i], pair)
        out_ref[:, my_head] = stage[1 + i, mine]
    recv(mix_land, mix_sem.at[3, 0])
    mixed_out[...] = (mix_keep[1] + mix_land[...].astype(F32)).astype(BF)
    for step in range(NY):
        for far in range(2):
            k = core if far == 0 else other
            if not (step == 0 and far == 0):
                recv(dw_land.at[step, k], dwy_sem.at[step, k])
    for k in range(2):
        dw_out[:, k * HD:(k + 1) * HD] = sum(dw_land[s, k].astype(F32) for s in range(NY)).astype(BF)
    for i, out_ref in enumerate((dq_out, dk_out, dv_out)):
        recv(out_ref.at[:, their_head], out_sem.at[i])
    for make, cond in sent:
        when(cond, lambda: make().wait_send())


def finish(*refs):
    ins, outs, held, sem = refs[:5], refs[5:10], refs[10:15], refs[15]
    first = [pltpu.make_async_copy(a, b, sem.at[0, i]) for i, (a, b) in enumerate(zip(ins, held))]
    second = [pltpu.make_async_copy(a, b, sem.at[1, i]) for i, (a, b) in enumerate(zip(held, outs))]
    for copy in first:
        copy.start()
    for a, b in zip(first, second):
        a.wait()
        b.start()
    for copy in second:
        copy.wait()


SENDS = 128


def body(queries, keys, values, out_grad, out_weight):
    block = jax.ShapeDtypeStruct((HALF, HALF), BF)
    dma = pltpu.SemaphoreType.DMA
    vmem = pltpu.VMEM
    results = pl.pallas_call(
        kernel,
        out_shape=(block, block, block, block, jax.ShapeDtypeStruct((32, HALF), BF)),
        in_specs=[pl.BlockSpec(memory_space=pltpu.HBM)] * 5,
        out_specs=[pl.BlockSpec(memory_space=pltpu.VMEM)] * 5,
        scratch_shapes=[
            vmem((HALF, HALF), BF),
            vmem((HALF, HALF), BF),
            vmem((HALF, HALF), BF),
            vmem((HALF, HALF), BF),
            vmem((HALF, 2048), BF),
            vmem((4, 5, TOK, HD), BF),
            vmem((8, HALF, HALF), BF),
            vmem((8, HALF, HALF), BF),
            vmem((5, 8, HD), F32),
            vmem((10, HALF, TOK), F32),
            vmem((1, TOK), F32),
            vmem((1, TOK), F32),
            vmem((HD, TOK), F32),
            vmem((HD, TOK), BF),
            vmem((TOK, HD), BF),
            vmem((HALF, HALF), BF),
            vmem((HD, TOK), F32),
            vmem((TOK, HD), F32),
            vmem((TOK, HD), F32),
            vmem((3, TOK, HD), BF),
            vmem((3, 2, HALF, HALF), BF),
            vmem((3, 2, HALF, HALF), BF),
            vmem((2, HALF, HALF), F32),
            vmem((HALF, HALF), BF),
            vmem((HALF, HALF), BF),
            vmem((NZ, HD, HALF), BF),
            vmem((NZ, HD, HALF), BF),
            vmem((HALF, HD), BF),
            vmem((NY, 2, 32, HD), BF),
            dma((5,)),
            dma((SENDS,)),
            dma((4, 5, 2)),
            dma((5,)),
            dma((8,)),
            dma((8,)),
            dma((5,)),
            dma((4, 2)),
            dma((NZ,)),
            dma((NY, 2)),
            dma((3,)),
            pltpu.SemaphoreType.REGULAR((2,)),
        ],
        compiler_params=pltpu.CompilerParams(
            collective_id=0, has_side_effects=True, vmem_limit_bytes=60 * 2**20
        ),
    )(queries, keys, values, out_grad, out_weight)
    shapes = [jax.ShapeDtypeStruct(r.shape, BF) for r in results]
    *results, dw = pl.pallas_call(
        finish,
        out_shape=shapes,
        in_specs=[pl.BlockSpec(memory_space=pltpu.HBM)] * 5,
        out_specs=[pl.BlockSpec(memory_space=pltpu.HBM)] * 5,
        scratch_shapes=[vmem(r.shape, BF) for r in results] + [dma((2, 5))],
    )(*results)
    return (*results, dw.T)


def solution(mesh):
    placed = (
        P("frames", "heads"),
        P("frames", "heads"),
        P("frames", "heads"),
        P("frames", "heads"),
        P("heads", None),
    )
    return jax.shard_map(
        body,
        mesh=mesh,
        in_specs=placed,
        out_specs=(
            P("frames", "heads"),
            P("frames", "heads"),
            P("frames", "heads"),
            P("frames", "heads"),
            P("heads", "frames"),
        ),
        check_vma=False,
    )
```

```python
import jax
import jax.numpy as jnp
from jax import lax
from jax.experimental import pallas as pl
from jax.experimental.pallas import tpu as pltpu
from jax.sharding import PartitionSpec as P

MESH = pl.DeviceIdType.MESH
BF = jnp.bfloat16
F32 = jnp.float32

NZ = 8
NY = 4
NX = 4
CHIPS = NZ * NY
HD = 128
HALF = 256
TOK = 512
SCALE = HD ** (-0.5)
LOW = -1e30

K, V, Q, G = range(4)
DETOUR = (V,)


def nt(a, b):
    return lax.dot_general(a, b, (((1,), (1,)), ((), ())), preferred_element_type=F32)


def nn(a, b):
    return jnp.dot(a, b, preferred_element_type=F32)


def kernel(
    q_hbm, k_hbm, v_hbm, og_hbm, w_hbm,
    mixed_out, dq_out, dk_out, dv_out, dw_out,
    k_in, v_in, q_in, g_in, w_in,
    buf, og_mine, og_pair, stat, scores,
    m_ref, l_ref, acc, attn_t, attn_tok, attn_own,
    dq_acc, dk_acc, dv_acc, stage,
    mix_send, mix_recv, mix_keep, mix_tail, mix_land,
    dw_send, dw_recv, dw_part, dw_land, detour,
    load_sem, send_sem, tree_sem, core_sem, og_sem, ogp_sem, stat_sem,
    mix_sem, dwz_sem, dwy_sem, out_sem, detour_sem, plane_sem,
):
    f = lax.axis_index("frames")
    h = lax.axis_index("heads")
    chip = lax.div(f, 2)
    core = lax.rem(f, 2)
    other = 1 - core
    z = lax.div(chip, NY)
    y = lax.rem(chip, NY)
    ylo = lax.div(h, NX)
    x = lax.rem(h, NX)

    def at(c, k):
        return (c * 2 + k, h)

    def along_x(step):
        return (f, ylo * NX + lax.rem(x + step + NX, NX))

    pair = (f + 1 - 2 * core, h)
    across = (f, (1 - ylo) * NX + x)
    mine = pl.ds(pl.multiple_of(core * HALF, HALF), HALF)
    theirs = pl.ds(pl.multiple_of(other * HALF, HALF), HALF)
    my_head = pl.ds(pl.multiple_of(core * HD, HD), HD)
    their_head = pl.ds(pl.multiple_of(other * HD, HD), HD)

    loads = []
    for i, (src, dst) in enumerate((
        (og_hbm, og_mine.at[h]), (k_hbm, k_in), (v_hbm, v_in), (q_hbm, q_in), (w_hbm, w_in),
    )):
        copy = pltpu.make_async_copy(src, dst, load_sem.at[i])
        copy.start()
        loads.append(copy)

    barrier = pltpu.get_barrier_semaphore()

    def in_reach(step):
        return (chip + step >= 0) & (chip + step < CHIPS)

    def greet(device):
        pl.semaphore_signal(barrier, inc=1, device_id=device, device_id_type=MESH)

    peers = [pair, across, along_x(1), along_x(2), along_x(3)]
    for step in range(1, NY):
        for k in range(2):
            peers.append(at(z * NY + lax.rem(y + step, NY), k))
    for peer in peers:
        greet(peer)
    expected = len(peers)
    for step in (1, -1, 2, -2, NY, -NY):
        def greet_chip(step=step):
            for k in (0, 1) if abs(step) == 1 else (core,):
                greet(at(chip + step, k))

        pl.when(in_reach(step))(greet_chip)
        expected = expected + jnp.where(in_reach(step), 2 if abs(step) == 1 else 1, 0)
    pl.semaphore_wait(barrier, expected)

    def tell(way, step, cond):
        pl.when(cond)(lambda: pl.semaphore_signal(
            plane_sem.at[way], inc=1, device_id=at(chip + step, core), device_id_type=MESH))

    tell(0, NY, z == 0)
    tell(1, -NY, z == NZ - 1)

    def hear_planes(i):
        @pl.when(z == i + 1)
        def _():
            pl.semaphore_wait(plane_sem.at[0], 1)

        tell(0, NY, (z == i + 1) & (z < NZ - 1))

        @pl.when(z == NZ - 2 - i)
        def _():
            pl.semaphore_wait(plane_sem.at[1], 1)

        tell(1, -NY, (z == NZ - 2 - i) & (z > 0))

    sent = []

    def when(cond, fn):
        if cond is None:
            fn()
        else:
            pl.when(cond)(fn)

    def send(src, dst, sem, device, cond=None):
        slot = len(sent)

        def make():
            return pltpu.make_async_remote_copy(
                src_ref=src, dst_ref=dst, send_sem=send_sem.at[slot], recv_sem=sem,
                device_id=device, device_id_type=MESH,
            )

        sent.append((make, cond))
        when(cond, lambda: make().start())

    def recv(dst, sem, cond=None):
        when(cond, lambda: pltpu.make_async_remote_copy(
            src_ref=dst, dst_ref=dst, send_sem=send_sem.at[0], recv_sem=sem,
            device_id=pair, device_id_type=MESH,
        ).wait_recv())

    def rows(j):
        return pl.ds(j * HALF, HALF)

    def spread(t, src):
        for step, slot in ((1, 1), (-1, 3)):
            cond = chip < CHIPS - 1 if step > 0 else chip > 0
            for k in range(2):
                send(src.at[:, pl.ds(k * HD, HD)], buf.at[t, slot, mine], tree_sem.at[t, slot, core],
                     at(chip + step, k), cond)
        if t in DETOUR:
            i = DETOUR.index(t)
            for end, step, j in ((0, 3, 1), (CHIPS - 1, -3, 0)):
                for k in range(2):
                    send(src.at[:, pl.ds(k * HD, HD)], detour.at[i], detour_sem.at[i],
                         at(chip + step, k), (chip == end) & (core == j))

    def chunk(t, slot, j):
        return buf.at[t, slot, rows(j)], tree_sem.at[t, slot, j]

    def arrive(t, slot, j, cond):
        recv(*chunk(t, slot, j), cond)

    def pass_on(t, slot, j, to_slot, step, cond):
        dst, sem = chunk(t, to_slot, j)
        send(buf.at[t, slot, rows(j)], dst, sem, at(chip + step, core), cond)

    has_left, has_right = chip >= 1, chip <= CHIPS - 2
    inner = has_left & has_right

    def relay_near(t):
        arrive(t, 1, 0, has_left)
        pass_on(t, 1, 0, 0, 1, inner)
        arrive(t, 3, 1, has_right)
        pass_on(t, 3, 1, 4, -1, inner)
        pass_on(t, 1, 0, 4, -3, chip == CHIPS - 1)
        pass_on(t, 3, 1, 0, 3, chip == 0)
        arrive(t, 1, 1, has_left)
        arrive(t, 3, 0, has_right)
        if t in DETOUR:
            i = DETOUR.index(t)
            for middle, step, slot, j in ((3, -1, 0, 1), (CHIPS - 4, 1, 4, 0)):
                recv(detour.at[i], detour_sem.at[i], chip == middle)
                dst, sem = chunk(t, slot, j)
                send(detour.at[i], dst, sem, at(chip + step, core), chip == middle)
        else:
            pass_on(t, 1, 1, 0, 1, chip == 1)
            pass_on(t, 3, 0, 4, -1, chip == CHIPS - 2)

    def relay_both(t):
        for j in range(2):
            for slot, to_slot, step, cond, half in ((1, 0, 1, has_left, j), (3, 4, -1, has_right, 1 - j)):
                arrive(t, slot, half, cond)
                pass_on(t, slot, half, to_slot, step, inner)

    def relay_end(t):
        for j in range(2):
            arrive(t, 0, j, chip >= 2)
            arrive(t, 4, j, chip <= CHIPS - 3)

    def relay_far(t):
        arrive(t, 0, 0, chip >= 2)
        pass_on(t, 0, 0, 4, -NY, chip >= NY)
        arrive(t, 4, 1, chip <= CHIPS - 3)
        pass_on(t, 4, 1, 0, NY, chip <= CHIPS - 1 - NY)

    def relay_last(t):
        arrive(t, 0, 1, chip >= 2)
        arrive(t, 4, 0, chip <= CHIPS - 3)

    def live(slot):
        block = chip + slot - 2
        return (block >= 0) & (block < CHIPS)

    loads[0].wait()
    send(og_mine.at[h], og_mine.at[h], og_sem.at[h], along_x(1))
    send(og_mine.at[h], og_mine.at[h], og_sem.at[h], along_x(-1))
    loads[1].wait()
    send(k_in.at[:, their_head], buf.at[K, 2, mine], core_sem.at[K], pair)
    spread(K, k_in)
    loads[2].wait()
    send(v_in.at[:, their_head], buf.at[V, 2, mine], core_sem.at[V], pair)
    loads[3].wait()
    send(q_in.at[:, their_head], buf.at[Q, 2, mine], core_sem.at[Q], pair)
    spread(V, v_in)
    send(og_mine.at[h], og_mine.at[h], og_sem.at[h], across)
    send(og_mine.at[h], og_pair.at[h], ogp_sem.at[h], pair)
    buf[K, 2, mine] = k_in[:, my_head]
    buf[V, 2, mine] = v_in[:, my_head]
    buf[Q, 2, mine] = q_in[:, my_head]
    m_ref[...] = jnp.full_like(m_ref, LOW)
    l_ref[...] = jnp.zeros_like(l_ref)
    acc[...] = jnp.zeros_like(acc)
    dq_acc[...] = jnp.zeros_like(dq_acc)
    dk_acc[...] = jnp.zeros_like(dk_acc)
    dv_acc[...] = jnp.zeros_like(dv_acc)

    def og_take(b):
        recv(og_mine.at[b], og_sem.at[b])
        send(og_mine.at[b], og_pair.at[b], ogp_sem.at[b], pair)

    def og_on(b, step):
        send(og_mine.at[b], og_mine.at[b], og_sem.at[b], along_x(step))

    def block_of(row, step):
        return row * NX + lax.rem(x + step + NX, NX)

    def near_mask(slot, key_frame, query_frame, shape):
        keys = lax.broadcasted_iota(jnp.int32, shape, 0) // HD + key_frame
        queries = lax.broadcasted_iota(jnp.int32, shape, 1) // HD + query_frame
        gap = (keys - queries) * jnp.where(slot == 0, 1, -1)
        return gap >= 0

    def attend(slot, j, masked):
        idx = slot * 2 + j
        keys = buf[K, slot, pl.ds(pl.multiple_of(j * HALF, HALF), HALF)]
        vals_t = buf[V, slot, pl.ds(pl.multiple_of(j * HALF, HALF), HALF)].T
        for part in range(2):
            lanes = pl.ds(part * HALF, HALF)
            s = nt(keys, buf[Q, 2, lanes]) * SCALE
            if masked:
                s = jnp.where(near_mask(slot, 2 * j, 2 * part, s.shape), s, LOW)
            scores[idx, :, lanes] = s
            old = m_ref[:, lanes]
            new = jnp.maximum(old, jnp.max(s, axis=0, keepdims=True))
            p = jnp.exp(s - new)
            fade = jnp.exp(old - new)
            m_ref[:, lanes] = new
            l_ref[:, lanes] = l_ref[:, lanes] * fade + jnp.sum(p, axis=0, keepdims=True)
            acc[:, lanes] = acc[:, lanes] * fade + nn(vals_t, p.astype(BF))

    def attend_all(pairs, masked):
        def step(i, carry):
            slot, j = pairs(i)
            pl.when(live(slot))(lambda: attend(slot, j, masked))
            return carry
        return step

    recv(buf.at[K, 2, theirs], core_sem.at[K])
    recv(buf.at[V, 2, theirs], core_sem.at[V])
    recv(buf.at[Q, 2, theirs], core_sem.at[Q])
    lax.fori_loop(0, 2, attend_all(lambda i: (2, i), False), 0)

    hear_planes(0)
    b = block_of(ylo, -1)
    og_take(b)
    og_on(b, 1)
    og_take(block_of(ylo, 1))
    hear_planes(1)
    relay_near(K)
    hear_planes(2)
    og_take(block_of(ylo, 2))
    relay_near(V)
    hear_planes(3)
    lax.fori_loop(0, 4, attend_all(lambda i: (1 + 2 * lax.rem(i, 2), lax.div(i, 2)), False), 0)
    b = block_of(1 - ylo, 0)
    og_take(b)
    og_on(b, 1)
    og_on(b, -1)
    hear_planes(4)
    relay_far(K)
    hear_planes(5)
    relay_far(V)
    spread(Q, q_in)
    hear_planes(6)
    lax.fori_loop(0, 2, attend_all(lambda i: (4 * i, i), True), 0)
    b = block_of(1 - ylo, 1)
    og_take(b)
    og_on(b, -1)
    og_take(block_of(1 - ylo, -1))
    relay_last(K)
    relay_last(V)
    lax.fori_loop(0, 2, attend_all(lambda i: (4 * i, 1 - i), True), 0)

    total = l_ref[...]
    out = acc[...] / total
    lse = m_ref[...] + jnp.log(total)
    m_ref[...] = lse
    acc[...] = out
    attn_t[...] = out.astype(BF)
    attn_tok[...] = out.T.astype(BF)
    send(attn_tok.at[theirs], attn_own.at[:, my_head], core_sem.at[4], pair)
    attn_own[:, my_head] = attn_tok[mine]

    def dw_blocks(row):
        for step in range(NX):
            b = block_of(row, step)
            recv(og_pair.at[b], ogp_sem.at[b])

        def dw_step(i, carry):
            plane = row * NX + i
            part = nn(attn_t[:, mine], og_mine[plane]) + nn(attn_t[:, theirs], og_pair[plane])
            dw_send[plane] = part.astype(BF)
            return carry

        lax.fori_loop(0, NX, dw_step, 0)
        for i in range(NX):
            plane = row * NX + i
            send(dw_send.at[plane], dw_recv.at[z], dwz_sem.at[z], at(plane * NY + y, core), z != plane)

    dw_blocks(ylo)
    og_take(block_of(1 - ylo, 2))
    loads[4].wait()

    grad = jnp.zeros((HALF, HALF), F32)

    def grad_step(i, total):
        cols = pl.ds(pl.multiple_of(i * HALF, HALF), HALF)
        return total + nt(og_mine[i], w_in[:, cols])

    g_in[...] = lax.fori_loop(0, 8, grad_step, grad).astype(BF)
    buf[G, 2, mine] = g_in[:, my_head]
    send(g_in.at[:, their_head], buf.at[G, 2, mine], core_sem.at[G], pair)

    relay_near(Q)
    spread(G, g_in)
    dw_blocks(1 - ylo)
    recv(buf.at[G, 2, theirs], core_sem.at[G])

    delta = jnp.sum(buf[G, 2].astype(F32).T * acc[...], axis=0, keepdims=True)
    lse = m_ref[...]
    for i in range(4):
        stat[2, i:i + 1] = lse[:, i * HD:(i + 1) * HD]
        stat[2, 4 + i:5 + i] = delta[:, i * HD:(i + 1) * HD]
    l_ref[...] = delta
    for step in (1, -1, 2, -2):
        cond = chip + step < CHIPS if step > 0 else chip + step >= 0
        send(stat.at[2], stat.at[2 - step], stat_sem.at[2 - step], at(chip + step, core), cond)

    recv(attn_own.at[:, their_head], core_sem.at[4])

    def mix_part(side, step):
        row = 1 - ylo if side == 0 else ylo
        cols = pl.ds(pl.multiple_of((row * NX + lax.rem(x + step, NX)) * HALF, HALF), HALF)
        return nn(attn_own[...], w_in[:, cols])

    def mix_out(side):
        def mix_step(i, carry):
            mix_send[i, side] = mix_part(side, i + 1).astype(BF)
            return carry

        lax.fori_loop(0, 3, mix_step, 0)
        for i in (1, 0, 2):
            send(mix_send.at[i, side], mix_recv.at[i, side], mix_sem.at[i, side], along_x(i + 1))

    mix_out(0)
    mix_out(1)
    mix_keep[0] = mix_part(0, 0)
    mix_keep[1] = mix_part(1, 0)

    def query_grad(i, carry):
        slot, j = lax.div(i, 2), lax.rem(i, 2)

        def run():
            at_rows = pl.ds(pl.multiple_of(j * HALF, HALF), HALF)
            keys_t = buf[K, slot, at_rows].T
            vals = buf[V, slot, at_rows]
            for part in range(2):
                lanes = pl.ds(part * HALF, HALF)
                p = jnp.exp(scores[i, :, lanes] - m_ref[:, lanes])
                d = nt(vals, buf[G, 2, lanes])
                ds = (p * (d - l_ref[:, lanes]) * SCALE).astype(BF)
                dq_acc[:, lanes] += nn(keys_t, ds)

        pl.when(live(slot))(run)
        return carry

    def collect(slot, j, masked):
        at_rows = pl.ds(pl.multiple_of(j * HALF, HALF), HALF)
        qs = buf[Q, slot, at_rows]
        gs = buf[G, slot, at_rows]

        def row(first):
            return jnp.concatenate(
                [stat[slot, pl.ds(first + 2 * j, 1)], stat[slot, pl.ds(first + 2 * j + 1, 1)]], axis=1)

        lse_row, delta_row = row(0), row(4)
        for part in range(2):
            own = pl.ds(part * HALF, HALF)
            s = nt(buf[K, 2, own], qs) * SCALE
            p = jnp.exp(s - lse_row)
            if masked:
                p = jnp.where(near_mask(4 - slot, 2 * part, 2 * j, p.shape), p, 0.0)
            d = nt(buf[V, 2, own], gs)
            ds = (p * (d - delta_row) * SCALE).astype(BF)
            dv_acc[own] += nn(p.astype(BF), gs)
            dk_acc[own] += nn(ds, qs)

    def collect_all(pairs, masked):
        def step(i, carry):
            slot, j = pairs(i)
            pl.when(live(slot))(lambda: collect(slot, j, masked))
            return carry
        return step

    def query_some(first, last):
        lax.fori_loop(first, last, query_grad, 0)

    def collect_some(count, pairs, masked):
        lax.fori_loop(0, count, collect_all(pairs, masked), 0)

    query_some(0, 4)
    relay_far(Q)
    query_some(4, 8)
    collect_some(2, lambda i: (2, i), False)
    relay_both(G)
    for slot in (1, 3, 0, 4):
        recv(stat.at[slot], stat_sem.at[slot], live(slot))
    collect_some(4, lambda i: (1 + 2 * lax.rem(i, 2), lax.div(i, 2)), False)

    def mix_sum(side):
        for i in range(3):
            recv(mix_recv.at[i, side], mix_sem.at[i, side])
        return mix_keep[side] + sum(mix_recv[i, side].astype(F32) for i in range(3))

    mix_tail[...] = mix_sum(0).astype(BF)
    send(mix_tail, mix_land, mix_sem.at[3, 0], across)
    query_some(8, 10)
    stage[0] = dq_acc[...].T.astype(BF)
    send(stage.at[0, theirs], dq_out.at[:, my_head], out_sem.at[0], pair)
    dq_out[:, my_head] = stage[0, mine]
    dw_recv[z] = dw_send[z]
    for plane in range(NZ):
        recv(dw_recv.at[plane], dwz_sem.at[plane], z != plane)
    part = dw_recv[0].astype(F32)
    for plane in range(1, NZ):
        part = part + dw_recv[plane].astype(F32)
    dw_part[...] = part.T.astype(BF)

    def cut(yy, k):
        return pl.ds(pl.multiple_of((yy * 2 + k) * 32, 32), 32)

    for step in range(NY):
        yy = lax.rem(y + step, NY)
        for far in range(2):
            k = core if far == 0 else other
            if step == 0 and far == 0:
                dw_land[0, core] = dw_part[cut(yy, k)]
            else:
                send(dw_part.at[cut(yy, k)], dw_land.at[step, core], dwy_sem.at[step, core],
                     at(z * NY + yy, k))

    relay_last(Q)
    relay_end(G)
    collect_some(4, lambda i: (4 * lax.rem(i, 2), lax.div(i, 2)), True)
    for i, (total_ref, out_ref) in enumerate(((dk_acc, dk_out), (dv_acc, dv_out))):
        stage[1 + i] = total_ref[...].astype(BF)
        send(stage.at[1 + i, theirs], out_ref.at[:, my_head], out_sem.at[1 + i], pair)
        out_ref[:, my_head] = stage[1 + i, mine]

    total = mix_sum(1)
    recv(mix_land, mix_sem.at[3, 0])
    mixed_out[...] = (total + mix_land[...].astype(F32)).astype(BF)
    for step in range(NY):
        for far in range(2):
            k = core if far == 0 else other
            if not (step == 0 and far == 0):
                recv(dw_land.at[step, k], dwy_sem.at[step, k])
    for k in range(2):
        dw_out[:, k * HD:(k + 1) * HD] = sum(dw_land[s, k].astype(F32) for s in range(NY)).astype(BF)
    for i, out_ref in enumerate((dq_out, dk_out, dv_out)):
        recv(out_ref.at[:, their_head], out_sem.at[i])
    assert len(sent) <= SENDS
    for make, cond in sent:
        when(cond, lambda: make().wait_send())


def finish(*refs):
    ins, outs, sem = refs[:5], refs[5:10], refs[10]
    copies = [pltpu.make_async_copy(a, b, sem.at[i]) for i, (a, b) in enumerate(zip(ins, outs))]
    for copy in copies:
        copy.start()
    for copy in copies:
        copy.wait()


SENDS = 136


def body(queries, keys, values, out_grad, out_weight):
    dma = pltpu.SemaphoreType.DMA
    vmem = pltpu.VMEM
    results = pl.pallas_call(
        kernel,
        out_shape=(*(pltpu.VMEM((HALF, HALF), BF) for _ in range(4)), pltpu.VMEM((32, HALF), BF)),
        in_specs=[pl.BlockSpec(memory_space=pltpu.HBM)] * 5,
        out_specs=[pl.BlockSpec(memory_space=pltpu.VMEM)] * 5,
        scratch_shapes=[
            vmem((HALF, HALF), BF),
            vmem((HALF, HALF), BF),
            vmem((HALF, HALF), BF),
            vmem((HALF, HALF), BF),
            vmem((HALF, 2048), BF),
            vmem((4, 5, TOK, HD), BF),
            vmem((8, HALF, HALF), BF),
            vmem((8, HALF, HALF), BF),
            vmem((5, 8, HD), F32),
            vmem((10, HALF, TOK), F32),
            vmem((1, TOK), F32),
            vmem((1, TOK), F32),
            vmem((HD, TOK), F32),
            vmem((HD, TOK), BF),
            vmem((TOK, HD), BF),
            vmem((HALF, HALF), BF),
            vmem((HD, TOK), F32),
            vmem((TOK, HD), F32),
            vmem((TOK, HD), F32),
            vmem((3, TOK, HD), BF),
            vmem((3, 2, HALF, HALF), BF),
            vmem((3, 2, HALF, HALF), BF),
            vmem((2, HALF, HALF), F32),
            vmem((HALF, HALF), BF),
            vmem((HALF, HALF), BF),
            vmem((NZ, HD, HALF), BF),
            vmem((NZ, HD, HALF), BF),
            vmem((HALF, HD), BF),
            vmem((NY, 2, 32, HD), BF),
            vmem((1, HALF, HD), BF),
            dma((5,)),
            dma((SENDS,)),
            dma((4, 5, 2)),
            dma((5,)),
            dma((8,)),
            dma((8,)),
            dma((5,)),
            dma((4, 2)),
            dma((NZ,)),
            dma((NY, 2)),
            dma((3,)),
            dma((1,)),
            pltpu.SemaphoreType.REGULAR((2,)),
        ],
        compiler_params=pltpu.CompilerParams(
            collective_id=0, has_side_effects=True, vmem_limit_bytes=60 * 2**20
        ),
    )(queries, keys, values, out_grad, out_weight)
    shapes = [jax.ShapeDtypeStruct(r.shape, BF) for r in results]
    *results, dw = pl.pallas_call(
        finish,
        out_shape=shapes,
        in_specs=[pl.BlockSpec(memory_space=pltpu.VMEM)] * 5,
        out_specs=[pl.BlockSpec(memory_space=pltpu.HBM)] * 5,
        scratch_shapes=[dma((5,))],
    )(*(pltpu.with_memory_space_constraint(r, pltpu.VMEM) for r in results))
    return (*results, dw.T)


def solution(mesh):
    placed = (
        P("frames", "heads"),
        P("frames", "heads"),
        P("frames", "heads"),
        P("frames", "heads"),
        P("heads", None),
    )
    return jax.shard_map(
        body,
        mesh=mesh,
        in_specs=placed,
        out_specs=(
            P("frames", "heads"),
            P("frames", "heads"),
            P("frames", "heads"),
            P("frames", "heads"),
            P("heads", "frames"),
        ),
        check_vma=False,
    )
```

```python
import jax
import jax.numpy as jnp
from jax import lax
from jax.experimental import pallas as pl
from jax.experimental.pallas import tpu as pltpu
from jax.sharding import PartitionSpec as P

MESH = pl.DeviceIdType.MESH
BF = jnp.bfloat16
F32 = jnp.float32

NZ = 8
NY = 4
NX = 4
CHIPS = NZ * NY
HD = 128
HALF = 256
TOK = 512
SCALE = HD ** (-0.5)
LOW = -1e30

K, V, Q, G = range(4)
DETOUR = (V,)


def nt(a, b):
    return lax.dot_general(a, b, (((1,), (1,)), ((), ())), preferred_element_type=F32)


def nn(a, b):
    return jnp.dot(a, b, preferred_element_type=F32)


def kernel(
    q_hbm, k_hbm, v_hbm, og_hbm, w_hbm,
    mixed_out, dq_out, dk_out, dv_out, dw_out,
    k_in, v_in, q_in, g_in, w_in,
    buf, og_mine, og_pair, stat, scores,
    m_ref, l_ref, acc, attn_t, attn_tok, attn_own,
    dq_acc, dk_acc, dv_acc, stage,
    mix_send, mix_recv, mix_keep, mix_tail, mix_land,
    dw_send, dw_recv, dw_part, dw_land, detour,
    load_sem, send_sem, tree_sem, core_sem, og_sem, ogp_sem, stat_sem,
    mix_sem, dwz_sem, dwy_sem, out_sem, detour_sem, plane_sem,
):
    f = lax.axis_index("frames")
    h = lax.axis_index("heads")
    chip = lax.div(f, 2)
    core = lax.rem(f, 2)
    other = 1 - core
    z = lax.div(chip, NY)
    y = lax.rem(chip, NY)
    ylo = lax.div(h, NX)
    x = lax.rem(h, NX)

    def at(c, k):
        return (c * 2 + k, h)

    def along_x(step):
        return (f, ylo * NX + lax.rem(x + step + NX, NX))

    pair = (f + 1 - 2 * core, h)
    across = (f, (1 - ylo) * NX + x)
    mine = pl.ds(pl.multiple_of(core * HALF, HALF), HALF)
    theirs = pl.ds(pl.multiple_of(other * HALF, HALF), HALF)
    my_head = pl.ds(pl.multiple_of(core * HD, HD), HD)
    their_head = pl.ds(pl.multiple_of(other * HD, HD), HD)

    loads = []
    for i, (src, dst) in enumerate((
        (og_hbm, og_mine.at[h]), (k_hbm, k_in), (v_hbm, v_in), (q_hbm, q_in), (w_hbm, w_in),
    )):
        copy = pltpu.make_async_copy(src, dst, load_sem.at[i])
        copy.start()
        loads.append(copy)

    barrier = pltpu.get_barrier_semaphore()

    def in_reach(step):
        return (chip + step >= 0) & (chip + step < CHIPS)

    def greet(device):
        pl.semaphore_signal(barrier, inc=1, device_id=device, device_id_type=MESH)

    peers = [pair, across, along_x(1), along_x(2), along_x(3)]
    for step in range(1, NY):
        for k in range(2):
            peers.append(at(z * NY + lax.rem(y + step, NY), k))
    for peer in peers:
        greet(peer)
    expected = len(peers)
    for step in (1, -1, 2, -2, NY, -NY):
        def greet_chip(step=step):
            for k in (0, 1) if abs(step) == 1 else (core,):
                greet(at(chip + step, k))

        pl.when(in_reach(step))(greet_chip)
        expected = expected + jnp.where(in_reach(step), 2 if abs(step) == 1 else 1, 0)
    pl.semaphore_wait(barrier, expected)

    def tell(way, step, cond):
        pl.when(cond)(lambda: pl.semaphore_signal(
            plane_sem.at[way], inc=1, device_id=at(chip + step, core), device_id_type=MESH))

    tell(0, NY, z == 0)
    tell(1, -NY, z == NZ - 1)

    def hear_planes(i):
        @pl.when(z == i + 1)
        def _():
            pl.semaphore_wait(plane_sem.at[0], 1)

        tell(0, NY, (z == i + 1) & (z < NZ - 1))

        @pl.when(z == NZ - 2 - i)
        def _():
            pl.semaphore_wait(plane_sem.at[1], 1)

        tell(1, -NY, (z == NZ - 2 - i) & (z > 0))

    sent = []

    def when(cond, fn):
        if cond is None:
            fn()
        else:
            pl.when(cond)(fn)

    def send(src, dst, sem, device, cond=None):
        slot = len(sent)

        def make():
            return pltpu.make_async_remote_copy(
                src_ref=src, dst_ref=dst, send_sem=send_sem.at[slot], recv_sem=sem,
                device_id=device, device_id_type=MESH,
            )

        sent.append((make, cond))
        when(cond, lambda: make().start())

    def recv(dst, sem, cond=None):
        when(cond, lambda: pltpu.make_async_remote_copy(
            src_ref=dst, dst_ref=dst, send_sem=send_sem.at[0], recv_sem=sem,
            device_id=pair, device_id_type=MESH,
        ).wait_recv())

    def rows(j):
        return pl.ds(j * HALF, HALF)

    def spread(t, src):
        for step, slot in ((1, 1), (-1, 3)):
            cond = chip < CHIPS - 1 if step > 0 else chip > 0
            for k in range(2):
                send(src.at[:, pl.ds(k * HD, HD)], buf.at[t, slot, mine], tree_sem.at[t, slot, core],
                     at(chip + step, k), cond)
        if t in DETOUR:
            i = DETOUR.index(t)
            for end, step, j in ((0, 3, 1), (CHIPS - 1, -3, 0)):
                for k in range(2):
                    send(src.at[:, pl.ds(k * HD, HD)], detour.at[i], detour_sem.at[i],
                         at(chip + step, k), (chip == end) & (core == j))

    def chunk(t, slot, j):
        return buf.at[t, slot, rows(j)], tree_sem.at[t, slot, j]

    def arrive(t, slot, j, cond):
        recv(*chunk(t, slot, j), cond)

    def pass_on(t, slot, j, to_slot, step, cond):
        dst, sem = chunk(t, to_slot, j)
        send(buf.at[t, slot, rows(j)], dst, sem, at(chip + step, core), cond)

    has_left, has_right = chip >= 1, chip <= CHIPS - 2
    inner = has_left & has_right

    def relay_near(t):
        arrive(t, 1, 0, has_left)
        pass_on(t, 1, 0, 0, 1, inner)
        arrive(t, 3, 1, has_right)
        pass_on(t, 3, 1, 4, -1, inner)
        pass_on(t, 1, 0, 4, -3, chip == CHIPS - 1)
        pass_on(t, 3, 1, 0, 3, chip == 0)
        arrive(t, 1, 1, has_left)
        arrive(t, 3, 0, has_right)
        if t in DETOUR:
            i = DETOUR.index(t)
            for middle, step, slot, j in ((3, -1, 0, 1), (CHIPS - 4, 1, 4, 0)):
                recv(detour.at[i], detour_sem.at[i], chip == middle)
                dst, sem = chunk(t, slot, j)
                send(detour.at[i], dst, sem, at(chip + step, core), chip == middle)
        else:
            pass_on(t, 1, 1, 0, 1, chip == 1)
            pass_on(t, 3, 0, 4, -1, chip == CHIPS - 2)

    def relay_both(t):
        for j in range(2):
            for slot, to_slot, step, cond, half in ((1, 0, 1, has_left, j), (3, 4, -1, has_right, 1 - j)):
                arrive(t, slot, half, cond)
                pass_on(t, slot, half, to_slot, step, inner)

    def relay_end(t):
        for j in range(2):
            arrive(t, 0, j, chip >= 2)
            arrive(t, 4, j, chip <= CHIPS - 3)

    def relay_far(t):
        arrive(t, 0, 0, chip >= 2)
        pass_on(t, 0, 0, 4, -NY, chip >= NY)
        arrive(t, 4, 1, chip <= CHIPS - 3)
        pass_on(t, 4, 1, 0, NY, chip <= CHIPS - 1 - NY)

    def relay_last(t):
        arrive(t, 0, 1, chip >= 2)
        arrive(t, 4, 0, chip <= CHIPS - 3)

    def live(slot):
        block = chip + slot - 2
        return (block >= 0) & (block < CHIPS)

    loads[0].wait()
    send(og_mine.at[h], og_mine.at[h], og_sem.at[h], along_x(1))
    send(og_mine.at[h], og_mine.at[h], og_sem.at[h], along_x(-1))
    loads[1].wait()
    send(k_in.at[:, their_head], buf.at[K, 2, mine], core_sem.at[K], pair)
    spread(K, k_in)
    loads[2].wait()
    send(v_in.at[:, their_head], buf.at[V, 2, mine], core_sem.at[V], pair)
    loads[3].wait()
    send(q_in.at[:, their_head], buf.at[Q, 2, mine], core_sem.at[Q], pair)
    spread(V, v_in)
    send(og_mine.at[h], og_mine.at[h], og_sem.at[h], across)
    send(og_mine.at[h], og_pair.at[h], ogp_sem.at[h], pair)
    buf[K, 2, mine] = k_in[:, my_head]
    buf[V, 2, mine] = v_in[:, my_head]
    buf[Q, 2, mine] = q_in[:, my_head]
    m_ref[...] = jnp.full_like(m_ref, LOW)
    l_ref[...] = jnp.zeros_like(l_ref)
    acc[...] = jnp.zeros_like(acc)
    dq_acc[...] = jnp.zeros_like(dq_acc)
    dk_acc[...] = jnp.zeros_like(dk_acc)
    dv_acc[...] = jnp.zeros_like(dv_acc)

    def og_take(b):
        recv(og_mine.at[b], og_sem.at[b])
        send(og_mine.at[b], og_pair.at[b], ogp_sem.at[b], pair)

    def og_on(b, step):
        send(og_mine.at[b], og_mine.at[b], og_sem.at[b], along_x(step))

    def block_of(row, step):
        return row * NX + lax.rem(x + step + NX, NX)

    def near_mask(slot, key_frame, query_frame, shape):
        keys = lax.broadcasted_iota(jnp.int32, shape, 0) // HD + key_frame
        queries = lax.broadcasted_iota(jnp.int32, shape, 1) // HD + query_frame
        gap = (keys - queries) * jnp.where(slot == 0, 1, -1)
        return gap >= 0

    def attend(slot, j, masked):
        idx = slot * 2 + j
        keys = buf[K, slot, pl.ds(pl.multiple_of(j * HALF, HALF), HALF)]
        vals_t = buf[V, slot, pl.ds(pl.multiple_of(j * HALF, HALF), HALF)].T
        for part in range(2):
            lanes = pl.ds(part * HALF, HALF)
            s = nt(keys, buf[Q, 2, lanes]) * SCALE
            if masked:
                s = jnp.where(near_mask(slot, 2 * j, 2 * part, s.shape), s, LOW)
            scores[idx, :, lanes] = s
            old = m_ref[:, lanes]
            new = jnp.maximum(old, jnp.max(s, axis=0, keepdims=True))
            p = jnp.exp(s - new)
            fade = jnp.exp(old - new)
            m_ref[:, lanes] = new
            l_ref[:, lanes] = l_ref[:, lanes] * fade + jnp.sum(p, axis=0, keepdims=True)
            acc[:, lanes] = acc[:, lanes] * fade + nn(vals_t, p.astype(BF))

    def attend_all(pairs, masked):
        def step(i, carry):
            slot, j = pairs(i)
            pl.when(live(slot))(lambda: attend(slot, j, masked))
            return carry
        return step

    recv(buf.at[K, 2, theirs], core_sem.at[K])
    recv(buf.at[V, 2, theirs], core_sem.at[V])
    recv(buf.at[Q, 2, theirs], core_sem.at[Q])
    lax.fori_loop(0, 2, attend_all(lambda i: (2, i), False), 0)

    hear_planes(0)
    b = block_of(ylo, -1)
    og_take(b)
    og_on(b, 1)
    og_take(block_of(ylo, 1))
    hear_planes(1)
    relay_near(K)
    hear_planes(2)
    og_take(block_of(ylo, 2))
    relay_near(V)
    hear_planes(3)
    lax.fori_loop(0, 4, attend_all(lambda i: (1 + 2 * lax.rem(i, 2), lax.div(i, 2)), False), 0)
    b = block_of(1 - ylo, 0)
    og_take(b)
    og_on(b, 1)
    og_on(b, -1)
    hear_planes(4)
    relay_far(K)
    relay_far(V)
    spread(Q, q_in)
    lax.fori_loop(0, 2, attend_all(lambda i: (4 * i, i), True), 0)
    b = block_of(1 - ylo, 1)
    og_take(b)
    og_on(b, -1)
    og_take(block_of(1 - ylo, -1))
    hear_planes(5)

    loads[4].wait()

    def grad_part(b):
        return nt(og_mine[b], w_in[:, pl.ds(pl.multiple_of(b * HALF, HALF), HALF)])

    grad = grad_part(block_of(ylo, 0))
    for row, step in ((ylo, 1), (ylo, 2), (ylo, 3), (1 - ylo, 0), (1 - ylo, 1), (1 - ylo, 3)):
        grad = grad + grad_part(block_of(row, step))
    mix_keep[0] = grad
    relay_last(K)
    relay_last(V)
    lax.fori_loop(0, 2, attend_all(lambda i: (4 * i, 1 - i), True), 0)

    total = l_ref[...]
    out = acc[...] / total
    lse = m_ref[...] + jnp.log(total)
    m_ref[...] = lse
    acc[...] = out
    attn_t[...] = out.astype(BF)
    attn_tok[...] = out.T.astype(BF)
    send(attn_tok.at[theirs], attn_own.at[:, my_head], core_sem.at[4], pair)
    attn_own[:, my_head] = attn_tok[mine]

    def dw_blocks(row):
        for step in range(NX):
            b = block_of(row, step)
            recv(og_pair.at[b], ogp_sem.at[b])

        def dw_step(i, carry):
            plane = row * NX + i
            part = nn(attn_t[:, mine], og_mine[plane]) + nn(attn_t[:, theirs], og_pair[plane])
            dw_send[plane] = part.astype(BF)
            return carry

        lax.fori_loop(0, NX, dw_step, 0)
        for i in range(NX):
            plane = row * NX + i
            send(dw_send.at[plane], dw_recv.at[z], dwz_sem.at[z], at(plane * NY + y, core), z != plane)

    og_take(block_of(1 - ylo, 2))
    g_in[...] = (mix_keep[0] + grad_part(block_of(1 - ylo, 2))).astype(BF)
    buf[G, 2, mine] = g_in[:, my_head]
    send(g_in.at[:, their_head], buf.at[G, 2, mine], core_sem.at[G], pair)
    spread(G, g_in)
    hear_planes(6)
    dw_blocks(ylo)
    dw_blocks(1 - ylo)
    relay_near(Q)
    recv(buf.at[G, 2, theirs], core_sem.at[G])

    delta = jnp.sum(buf[G, 2].astype(F32).T * acc[...], axis=0, keepdims=True)
    lse = m_ref[...]
    for i in range(4):
        stat[2, i:i + 1] = lse[:, i * HD:(i + 1) * HD]
        stat[2, 4 + i:5 + i] = delta[:, i * HD:(i + 1) * HD]
    l_ref[...] = delta
    for step in (1, -1, 2, -2):
        cond = chip + step < CHIPS if step > 0 else chip + step >= 0
        send(stat.at[2], stat.at[2 - step], stat_sem.at[2 - step], at(chip + step, core), cond)

    recv(attn_own.at[:, their_head], core_sem.at[4])

    def mix_part(side, step):
        row = 1 - ylo if side == 0 else ylo
        cols = pl.ds(pl.multiple_of((row * NX + lax.rem(x + step, NX)) * HALF, HALF), HALF)
        return nn(attn_own[...], w_in[:, cols])

    def mix_out(side):
        def mix_step(i, carry):
            mix_send[i, side] = mix_part(side, i + 1).astype(BF)
            return carry

        lax.fori_loop(0, 3, mix_step, 0)
        for i in (1, 0, 2):
            send(mix_send.at[i, side], mix_recv.at[i, side], mix_sem.at[i, side], along_x(i + 1))

    mix_out(0)
    mix_out(1)
    mix_keep[0] = mix_part(0, 0)
    mix_keep[1] = mix_part(1, 0)

    def query_grad(i, carry):
        slot, j = lax.div(i, 2), lax.rem(i, 2)

        def run():
            at_rows = pl.ds(pl.multiple_of(j * HALF, HALF), HALF)
            keys_t = buf[K, slot, at_rows].T
            vals = buf[V, slot, at_rows]
            for part in range(2):
                lanes = pl.ds(part * HALF, HALF)
                p = jnp.exp(scores[i, :, lanes] - m_ref[:, lanes])
                d = nt(vals, buf[G, 2, lanes])
                ds = (p * (d - l_ref[:, lanes]) * SCALE).astype(BF)
                dq_acc[:, lanes] += nn(keys_t, ds)

        pl.when(live(slot))(run)
        return carry

    def collect(slot, j, masked):
        at_rows = pl.ds(pl.multiple_of(j * HALF, HALF), HALF)
        qs = buf[Q, slot, at_rows]
        gs = buf[G, slot, at_rows]

        def row(first):
            return jnp.concatenate(
                [stat[slot, pl.ds(first + 2 * j, 1)], stat[slot, pl.ds(first + 2 * j + 1, 1)]], axis=1)

        lse_row, delta_row = row(0), row(4)
        for part in range(2):
            own = pl.ds(part * HALF, HALF)
            s = nt(buf[K, 2, own], qs) * SCALE
            p = jnp.exp(s - lse_row)
            if masked:
                p = jnp.where(near_mask(4 - slot, 2 * part, 2 * j, p.shape), p, 0.0)
            d = nt(buf[V, 2, own], gs)
            ds = (p * (d - delta_row) * SCALE).astype(BF)
            dv_acc[own] += nn(p.astype(BF), gs)
            dk_acc[own] += nn(ds, qs)

    def collect_all(pairs, masked):
        def step(i, carry):
            slot, j = pairs(i)
            pl.when(live(slot))(lambda: collect(slot, j, masked))
            return carry
        return step

    def query_some(first, last):
        lax.fori_loop(first, last, query_grad, 0)

    def collect_some(count, pairs, masked):
        lax.fori_loop(0, count, collect_all(pairs, masked), 0)

    query_some(0, 4)
    relay_both(G)
    collect_some(2, lambda i: (2, i), False)
    query_some(4, 6)
    relay_far(Q)
    for slot in (1, 3, 0, 4):
        recv(stat.at[slot], stat_sem.at[slot], live(slot))
    collect_some(4, lambda i: (1 + 2 * lax.rem(i, 2), lax.div(i, 2)), False)

    def mix_sum(side):
        for i in range(3):
            recv(mix_recv.at[i, side], mix_sem.at[i, side])
        return mix_keep[side] + sum(mix_recv[i, side].astype(F32) for i in range(3))

    mix_tail[...] = mix_sum(0).astype(BF)
    send(mix_tail, mix_land, mix_sem.at[3, 0], across)
    query_some(6, 10)
    stage[0] = dq_acc[...].T.astype(BF)
    send(stage.at[0, theirs], dq_out.at[:, my_head], out_sem.at[0], pair)
    dq_out[:, my_head] = stage[0, mine]
    dw_recv[z] = dw_send[z]
    for plane in range(NZ):
        recv(dw_recv.at[plane], dwz_sem.at[plane], z != plane)
    part = dw_recv[0].astype(F32)
    for plane in range(1, NZ):
        part = part + dw_recv[plane].astype(F32)
    dw_part[...] = part.T.astype(BF)

    def cut(yy, k):
        return pl.ds(pl.multiple_of((yy * 2 + k) * 32, 32), 32)

    for step in range(NY):
        yy = lax.rem(y + step, NY)
        for far in range(2):
            k = core if far == 0 else other
            if step == 0 and far == 0:
                dw_land[0, core] = dw_part[cut(yy, k)]
            else:
                send(dw_part.at[cut(yy, k)], dw_land.at[step, core], dwy_sem.at[step, core],
                     at(z * NY + yy, k))

    relay_last(Q)
    relay_end(G)
    collect_some(4, lambda i: (4 * lax.rem(i, 2), lax.div(i, 2)), True)
    for i, (total_ref, out_ref) in enumerate(((dk_acc, dk_out), (dv_acc, dv_out))):
        stage[1 + i] = total_ref[...].astype(BF)
        send(stage.at[1 + i, theirs], out_ref.at[:, my_head], out_sem.at[1 + i], pair)
        out_ref[:, my_head] = stage[1 + i, mine]

    total = mix_sum(1)
    recv(mix_land, mix_sem.at[3, 0])
    mixed_out[...] = (total + mix_land[...].astype(F32)).astype(BF)
    for step in range(NY):
        for far in range(2):
            k = core if far == 0 else other
            if not (step == 0 and far == 0):
                recv(dw_land.at[step, k], dwy_sem.at[step, k])
    for k in range(2):
        dw_out[:, k * HD:(k + 1) * HD] = sum(dw_land[s, k].astype(F32) for s in range(NY)).astype(BF)
    for i, out_ref in enumerate((dq_out, dk_out, dv_out)):
        recv(out_ref.at[:, their_head], out_sem.at[i])
    assert len(sent) <= SENDS
    for make, cond in sent:
        when(cond, lambda: make().wait_send())


def finish(*refs):
    ins, outs, sem = refs[:5], refs[5:10], refs[10]
    copies = [pltpu.make_async_copy(a, b, sem.at[i]) for i, (a, b) in enumerate(zip(ins, outs))]
    for copy in copies:
        copy.start()
    for copy in copies:
        copy.wait()


SENDS = 136


def body(queries, keys, values, out_grad, out_weight):
    dma = pltpu.SemaphoreType.DMA
    vmem = pltpu.VMEM
    results = pl.pallas_call(
        kernel,
        out_shape=(*(pltpu.VMEM((HALF, HALF), BF) for _ in range(4)), pltpu.VMEM((32, HALF), BF)),
        in_specs=[pl.BlockSpec(memory_space=pltpu.HBM)] * 5,
        out_specs=[pl.BlockSpec(memory_space=pltpu.VMEM)] * 5,
        scratch_shapes=[
            vmem((HALF, HALF), BF),
            vmem((HALF, HALF), BF),
            vmem((HALF, HALF), BF),
            vmem((HALF, HALF), BF),
            vmem((HALF, 2048), BF),
            vmem((4, 5, TOK, HD), BF),
            vmem((8, HALF, HALF), BF),
            vmem((8, HALF, HALF), BF),
            vmem((5, 8, HD), F32),
            vmem((10, HALF, TOK), F32),
            vmem((1, TOK), F32),
            vmem((1, TOK), F32),
            vmem((HD, TOK), F32),
            vmem((HD, TOK), BF),
            vmem((TOK, HD), BF),
            vmem((HALF, HALF), BF),
            vmem((HD, TOK), F32),
            vmem((TOK, HD), F32),
            vmem((TOK, HD), F32),
            vmem((3, TOK, HD), BF),
            vmem((3, 2, HALF, HALF), BF),
            vmem((3, 2, HALF, HALF), BF),
            vmem((2, HALF, HALF), F32),
            vmem((HALF, HALF), BF),
            vmem((HALF, HALF), BF),
            vmem((NZ, HD, HALF), BF),
            vmem((NZ, HD, HALF), BF),
            vmem((HALF, HD), BF),
            vmem((NY, 2, 32, HD), BF),
            vmem((1, HALF, HD), BF),
            dma((5,)),
            dma((SENDS,)),
            dma((4, 5, 2)),
            dma((5,)),
            dma((8,)),
            dma((8,)),
            dma((5,)),
            dma((4, 2)),
            dma((NZ,)),
            dma((NY, 2)),
            dma((3,)),
            dma((1,)),
            pltpu.SemaphoreType.REGULAR((2,)),
        ],
        compiler_params=pltpu.CompilerParams(
            collective_id=0, has_side_effects=True, vmem_limit_bytes=60 * 2**20
        ),
    )(queries, keys, values, out_grad, out_weight)
    shapes = [jax.ShapeDtypeStruct(r.shape, BF) for r in results]
    *results, dw = pl.pallas_call(
        finish,
        out_shape=shapes,
        in_specs=[pl.BlockSpec(memory_space=pltpu.VMEM)] * 5,
        out_specs=[pl.BlockSpec(memory_space=pltpu.HBM)] * 5,
        scratch_shapes=[dma((5,))],
    )(*(pltpu.with_memory_space_constraint(r, pltpu.VMEM) for r in results))
    return (*results, dw.T)


def solution(mesh):
    placed = (
        P("frames", "heads"),
        P("frames", "heads"),
        P("frames", "heads"),
        P("frames", "heads"),
        P("heads", None),
    )
    return jax.shard_map(
        body,
        mesh=mesh,
        in_specs=placed,
        out_specs=(
            P("frames", "heads"),
            P("frames", "heads"),
            P("frames", "heads"),
            P("frames", "heads"),
            P("heads", "frames"),
        ),
        check_vma=False,
    )
```

```python
import jax
import jax.numpy as jnp
from jax import lax
from jax.experimental import pallas as pl
from jax.experimental.pallas import tpu as pltpu
from jax.sharding import PartitionSpec as P

MESH = pl.DeviceIdType.MESH
BF = jnp.bfloat16
F32 = jnp.float32

NZ = 8
NY = 4
NX = 4
CHIPS = NZ * NY
HD = 128
HALF = 256
TOK = 512
SCALE = HD ** (-0.5)
LOW = -1e30

K, V, Q, G = range(4)
DETOUR = (V, Q)


def nt(a, b):
    return lax.dot_general(a, b, (((1,), (1,)), ((), ())), preferred_element_type=F32)


def nn(a, b):
    return jnp.dot(a, b, preferred_element_type=F32)


def kernel(
    q_hbm, k_hbm, v_hbm, og_hbm, w_hbm,
    mixed_out, dq_out, dk_out, dv_out, dw_out,
    k_in, v_in, q_in, g_in, w_in,
    buf, og_mine, og_pair, stat, scores,
    m_ref, l_ref, acc, attn_t, attn_tok, attn_own,
    dq_acc, dk_acc, dv_acc, stage,
    mix_send, mix_recv, mix_keep, mix_tail, mix_land,
    dw_send, dw_recv, dw_part, dw_land, detour,
    load_sem, send_sem, tree_sem, core_sem, og_sem, ogp_sem, stat_sem,
    mix_sem, dwz_sem, dwy_sem, out_sem, detour_sem, plane_sem,
):
    f = lax.axis_index("frames")
    h = lax.axis_index("heads")
    chip = lax.div(f, 2)
    core = lax.rem(f, 2)
    other = 1 - core
    z = lax.div(chip, NY)
    y = lax.rem(chip, NY)
    ylo = lax.div(h, NX)
    x = lax.rem(h, NX)

    def at(c, k):
        return (c * 2 + k, h)

    def along_x(step):
        return (f, ylo * NX + lax.rem(x + step + NX, NX))

    pair = (f + 1 - 2 * core, h)
    across = (f, (1 - ylo) * NX + x)
    mine = pl.ds(pl.multiple_of(core * HALF, HALF), HALF)
    theirs = pl.ds(pl.multiple_of(other * HALF, HALF), HALF)
    my_head = pl.ds(pl.multiple_of(core * HD, HD), HD)
    their_head = pl.ds(pl.multiple_of(other * HD, HD), HD)

    loads = []
    for i, (src, dst) in enumerate((
        (og_hbm, og_mine.at[h]), (k_hbm, k_in), (v_hbm, v_in), (q_hbm, q_in), (w_hbm, w_in),
    )):
        copy = pltpu.make_async_copy(src, dst, load_sem.at[i])
        copy.start()
        loads.append(copy)

    barrier = pltpu.get_barrier_semaphore()

    def in_reach(step):
        return (chip + step >= 0) & (chip + step < CHIPS)

    def greet(device):
        pl.semaphore_signal(barrier, inc=1, device_id=device, device_id_type=MESH)

    peers = [pair, across, along_x(1), along_x(2), along_x(3)]
    for step in range(1, NY):
        for k in range(2):
            peers.append(at(z * NY + lax.rem(y + step, NY), k))
    for peer in peers:
        greet(peer)
    expected = len(peers)
    for step in (1, -1, 2, -2, NY, -NY):
        def greet_chip(step=step):
            for k in (0, 1) if abs(step) == 1 else (core,):
                greet(at(chip + step, k))

        pl.when(in_reach(step))(greet_chip)
        expected = expected + jnp.where(in_reach(step), 2 if abs(step) == 1 else 1, 0)
    pl.semaphore_wait(barrier, expected)

    def tell(way, step, cond):
        pl.when(cond)(lambda: pl.semaphore_signal(
            plane_sem.at[way], inc=1, device_id=at(chip + step, core), device_id_type=MESH))

    tell(0, NY, z == 0)
    tell(1, -NY, z == NZ - 1)

    def hear_planes(i):
        @pl.when(z == i + 1)
        def _():
            pl.semaphore_wait(plane_sem.at[0], 1)

        tell(0, NY, (z == i + 1) & (z < NZ - 1))

        @pl.when(z == NZ - 2 - i)
        def _():
            pl.semaphore_wait(plane_sem.at[1], 1)

        tell(1, -NY, (z == NZ - 2 - i) & (z > 0))

    sent = []

    def when(cond, fn):
        if cond is None:
            fn()
        else:
            pl.when(cond)(fn)

    def send(src, dst, sem, device, cond=None):
        slot = len(sent)

        def make():
            return pltpu.make_async_remote_copy(
                src_ref=src, dst_ref=dst, send_sem=send_sem.at[slot], recv_sem=sem,
                device_id=device, device_id_type=MESH,
            )

        sent.append((make, cond))
        when(cond, lambda: make().start())

    def recv(dst, sem, cond=None):
        when(cond, lambda: pltpu.make_async_remote_copy(
            src_ref=dst, dst_ref=dst, send_sem=send_sem.at[0], recv_sem=sem,
            device_id=pair, device_id_type=MESH,
        ).wait_recv())

    def rows(j):
        return pl.ds(j * HALF, HALF)

    def spread(t, src):
        for step, slot in ((1, 1), (-1, 3)):
            cond = chip < CHIPS - 1 if step > 0 else chip > 0
            for k in range(2):
                send(src.at[:, pl.ds(k * HD, HD)], buf.at[t, slot, mine], tree_sem.at[t, slot, core],
                     at(chip + step, k), cond)
        if t in DETOUR:
            i = DETOUR.index(t)
            for end, step, j in ((0, 3, 1), (CHIPS - 1, -3, 0)):
                for k in range(2):
                    send(src.at[:, pl.ds(k * HD, HD)], detour.at[i], detour_sem.at[i],
                         at(chip + step, k), (chip == end) & (core == j))

    def chunk(t, slot, j):
        return buf.at[t, slot, rows(j)], tree_sem.at[t, slot, j]

    def arrive(t, slot, j, cond):
        recv(*chunk(t, slot, j), cond)

    def pass_on(t, slot, j, to_slot, step, cond):
        dst, sem = chunk(t, to_slot, j)
        send(buf.at[t, slot, rows(j)], dst, sem, at(chip + step, core), cond)

    has_left, has_right = chip >= 1, chip <= CHIPS - 2
    inner = has_left & has_right

    def relay_near(t):
        arrive(t, 1, 0, has_left)
        pass_on(t, 1, 0, 0, 1, inner)
        arrive(t, 3, 1, has_right)
        pass_on(t, 3, 1, 4, -1, inner)
        pass_on(t, 1, 0, 4, -3, chip == CHIPS - 1)
        pass_on(t, 3, 1, 0, 3, chip == 0)
        arrive(t, 1, 1, has_left)
        arrive(t, 3, 0, has_right)
        if t in DETOUR:
            i = DETOUR.index(t)
            for middle, step, slot, j in ((3, -1, 0, 1), (CHIPS - 4, 1, 4, 0)):
                recv(detour.at[i], detour_sem.at[i], chip == middle)
                dst, sem = chunk(t, slot, j)
                send(detour.at[i], dst, sem, at(chip + step, core), chip == middle)
        else:
            pass_on(t, 1, 1, 0, 1, chip == 1)
            pass_on(t, 3, 0, 4, -1, chip == CHIPS - 2)

    def relay_both(t):
        for j in range(2):
            for slot, to_slot, step, cond, half in ((1, 0, 1, has_left, j), (3, 4, -1, has_right, 1 - j)):
                arrive(t, slot, half, cond)
                pass_on(t, slot, half, to_slot, step, inner)

    def relay_end(t):
        for j in range(2):
            arrive(t, 0, j, chip >= 2)
            arrive(t, 4, j, chip <= CHIPS - 3)

    def relay_far(t):
        arrive(t, 0, 0, chip >= 2)
        pass_on(t, 0, 0, 4, -NY, chip >= NY)
        arrive(t, 4, 1, chip <= CHIPS - 3)
        pass_on(t, 4, 1, 0, NY, chip <= CHIPS - 1 - NY)

    def relay_last(t):
        arrive(t, 0, 1, chip >= 2)
        arrive(t, 4, 0, chip <= CHIPS - 3)

    def live(slot):
        block = chip + slot - 2
        return (block >= 0) & (block < CHIPS)

    loads[0].wait()
    send(og_mine.at[h], og_mine.at[h], og_sem.at[h], along_x(1))
    send(og_mine.at[h], og_mine.at[h], og_sem.at[h], along_x(-1))
    loads[1].wait()
    send(k_in.at[:, their_head], buf.at[K, 2, mine], core_sem.at[K], pair)
    spread(K, k_in)
    loads[2].wait()
    send(v_in.at[:, their_head], buf.at[V, 2, mine], core_sem.at[V], pair)
    loads[3].wait()
    send(q_in.at[:, their_head], buf.at[Q, 2, mine], core_sem.at[Q], pair)
    spread(V, v_in)
    send(og_mine.at[h], og_mine.at[h], og_sem.at[h], across)
    send(og_mine.at[h], og_pair.at[h], ogp_sem.at[h], pair)
    buf[K, 2, mine] = k_in[:, my_head]
    buf[V, 2, mine] = v_in[:, my_head]
    buf[Q, 2, mine] = q_in[:, my_head]
    m_ref[...] = jnp.full_like(m_ref, LOW)
    l_ref[...] = jnp.zeros_like(l_ref)
    acc[...] = jnp.zeros_like(acc)
    dq_acc[...] = jnp.zeros_like(dq_acc)
    dk_acc[...] = jnp.zeros_like(dk_acc)
    dv_acc[...] = jnp.zeros_like(dv_acc)

    def og_take(b):
        recv(og_mine.at[b], og_sem.at[b])
        send(og_mine.at[b], og_pair.at[b], ogp_sem.at[b], pair)

    def og_on(b, step):
        send(og_mine.at[b], og_mine.at[b], og_sem.at[b], along_x(step))

    def block_of(row, step):
        return row * NX + lax.rem(x + step + NX, NX)

    def near_mask(slot, key_frame, query_frame, shape):
        keys = lax.broadcasted_iota(jnp.int32, shape, 0) // HD + key_frame
        queries = lax.broadcasted_iota(jnp.int32, shape, 1) // HD + query_frame
        gap = (keys - queries) * jnp.where(slot == 0, 1, -1)
        return gap >= 0

    def attend(slot, j, masked):
        idx = slot * 2 + j
        keys = buf[K, slot, pl.ds(pl.multiple_of(j * HALF, HALF), HALF)]
        vals_t = buf[V, slot, pl.ds(pl.multiple_of(j * HALF, HALF), HALF)].T
        for part in range(2):
            lanes = pl.ds(part * HALF, HALF)
            s = nt(keys, buf[Q, 2, lanes]) * SCALE
            if masked:
                s = jnp.where(near_mask(slot, 2 * j, 2 * part, s.shape), s, LOW)
            scores[idx, :, lanes] = s
            old = m_ref[:, lanes]
            new = jnp.maximum(old, jnp.max(s, axis=0, keepdims=True))
            p = jnp.exp(s - new)
            fade = jnp.exp(old - new)
            m_ref[:, lanes] = new
            l_ref[:, lanes] = l_ref[:, lanes] * fade + jnp.sum(p, axis=0, keepdims=True)
            acc[:, lanes] = acc[:, lanes] * fade + nn(vals_t, p.astype(BF))

    def attend_all(pairs, masked):
        def step(i, carry):
            slot, j = pairs(i)
            pl.when(live(slot))(lambda: attend(slot, j, masked))
            return carry
        return step

    recv(buf.at[K, 2, theirs], core_sem.at[K])
    recv(buf.at[V, 2, theirs], core_sem.at[V])
    recv(buf.at[Q, 2, theirs], core_sem.at[Q])
    lax.fori_loop(0, 2, attend_all(lambda i: (2, i), False), 0)

    hear_planes(0)
    b = block_of(ylo, -1)
    og_take(b)
    og_on(b, 1)
    og_take(block_of(ylo, 1))
    hear_planes(1)
    relay_near(K)
    hear_planes(2)
    og_take(block_of(ylo, 2))
    relay_near(V)
    hear_planes(3)
    lax.fori_loop(0, 4, attend_all(lambda i: (1 + 2 * lax.rem(i, 2), lax.div(i, 2)), False), 0)
    b = block_of(1 - ylo, 0)
    og_take(b)
    og_on(b, 1)
    og_on(b, -1)
    hear_planes(4)
    relay_far(K)
    relay_far(V)
    spread(Q, q_in)
    lax.fori_loop(0, 2, attend_all(lambda i: (4 * i, i), True), 0)
    b = block_of(1 - ylo, 1)
    og_take(b)
    og_on(b, -1)
    og_take(block_of(1 - ylo, -1))
    hear_planes(5)

    loads[4].wait()

    def grad_part(b):
        return nt(og_mine[b], w_in[:, pl.ds(pl.multiple_of(b * HALF, HALF), HALF)])

    grad = grad_part(block_of(ylo, 0))
    for row, step in ((ylo, 1), (ylo, 2), (ylo, 3), (1 - ylo, 0), (1 - ylo, 1), (1 - ylo, 3)):
        grad = grad + grad_part(block_of(row, step))
    mix_keep[0] = grad
    relay_last(K)
    relay_last(V)
    lax.fori_loop(0, 2, attend_all(lambda i: (4 * i, 1 - i), True), 0)

    total = l_ref[...]
    out = acc[...] / total
    lse = m_ref[...] + jnp.log(total)
    m_ref[...] = lse
    acc[...] = out
    attn_t[...] = out.astype(BF)
    attn_tok[...] = out.T.astype(BF)
    send(attn_tok.at[theirs], attn_own.at[:, my_head], core_sem.at[4], pair)
    attn_own[:, my_head] = attn_tok[mine]

    def dw_blocks(row):
        for step in range(NX):
            b = block_of(row, step)
            recv(og_pair.at[b], ogp_sem.at[b])

        def dw_step(i, carry):
            plane = row * NX + i
            part = nn(attn_t[:, mine], og_mine[plane]) + nn(attn_t[:, theirs], og_pair[plane])
            dw_send[plane] = part.astype(BF)
            return carry

        lax.fori_loop(0, NX, dw_step, 0)
        for i in range(NX):
            plane = row * NX + i
            send(dw_send.at[plane], dw_recv.at[z], dwz_sem.at[z], at(plane * NY + y, core), z != plane)

    og_take(block_of(1 - ylo, 2))
    g_in[...] = (mix_keep[0] + grad_part(block_of(1 - ylo, 2))).astype(BF)
    buf[G, 2, mine] = g_in[:, my_head]
    send(g_in.at[:, their_head], buf.at[G, 2, mine], core_sem.at[G], pair)
    spread(G, g_in)
    hear_planes(6)
    dw_blocks(ylo)
    dw_blocks(1 - ylo)
    relay_near(Q)
    recv(buf.at[G, 2, theirs], core_sem.at[G])

    delta = jnp.sum(buf[G, 2].astype(F32).T * acc[...], axis=0, keepdims=True)
    lse = m_ref[...]
    for i in range(4):
        stat[2, i:i + 1] = lse[:, i * HD:(i + 1) * HD]
        stat[2, 4 + i:5 + i] = delta[:, i * HD:(i + 1) * HD]
    l_ref[...] = delta
    for step in (1, -1, 2, -2):
        cond = chip + step < CHIPS if step > 0 else chip + step >= 0
        send(stat.at[2], stat.at[2 - step], stat_sem.at[2 - step], at(chip + step, core), cond)

    recv(attn_own.at[:, their_head], core_sem.at[4])

    def mix_part(side, step):
        row = 1 - ylo if side == 0 else ylo
        cols = pl.ds(pl.multiple_of((row * NX + lax.rem(x + step, NX)) * HALF, HALF), HALF)
        return nn(attn_own[...], w_in[:, cols])

    def mix_out(side):
        def mix_step(i, carry):
            mix_send[i, side] = mix_part(side, i + 1).astype(BF)
            return carry

        lax.fori_loop(0, 3, mix_step, 0)
        for i in (1, 0, 2):
            send(mix_send.at[i, side], mix_recv.at[i, side], mix_sem.at[i, side], along_x(i + 1))

    mix_out(0)
    mix_out(1)
    mix_keep[0] = mix_part(0, 0)
    mix_keep[1] = mix_part(1, 0)

    def query_grad(i, carry):
        slot, j = lax.div(i, 2), lax.rem(i, 2)

        def run():
            at_rows = pl.ds(pl.multiple_of(j * HALF, HALF), HALF)
            keys_t = buf[K, slot, at_rows].T
            vals = buf[V, slot, at_rows]
            for part in range(2):
                lanes = pl.ds(part * HALF, HALF)
                p = jnp.exp(scores[i, :, lanes] - m_ref[:, lanes])
                d = nt(vals, buf[G, 2, lanes])
                ds = (p * (d - l_ref[:, lanes]) * SCALE).astype(BF)
                dq_acc[:, lanes] += nn(keys_t, ds)

        pl.when(live(slot))(run)
        return carry

    def collect(slot, j, masked):
        at_rows = pl.ds(pl.multiple_of(j * HALF, HALF), HALF)
        qs = buf[Q, slot, at_rows]
        gs = buf[G, slot, at_rows]

        def row(first):
            return jnp.concatenate(
                [stat[slot, pl.ds(first + 2 * j, 1)], stat[slot, pl.ds(first + 2 * j + 1, 1)]], axis=1)

        lse_row, delta_row = row(0), row(4)
        for part in range(2):
            own = pl.ds(part * HALF, HALF)
            s = nt(buf[K, 2, own], qs) * SCALE
            p = jnp.exp(s - lse_row)
            if masked:
                p = jnp.where(near_mask(4 - slot, 2 * part, 2 * j, p.shape), p, 0.0)
            d = nt(buf[V, 2, own], gs)
            ds = (p * (d - delta_row) * SCALE).astype(BF)
            dv_acc[own] += nn(p.astype(BF), gs)
            dk_acc[own] += nn(ds, qs)

    def collect_all(pairs, masked):
        def step(i, carry):
            slot, j = pairs(i)
            pl.when(live(slot))(lambda: collect(slot, j, masked))
            return carry
        return step

    def query_some(first, last):
        lax.fori_loop(first, last, query_grad, 0)

    def collect_some(count, pairs, masked):
        lax.fori_loop(0, count, collect_all(pairs, masked), 0)

    query_some(0, 4)
    relay_both(G)
    collect_some(2, lambda i: (2, i), False)
    query_some(4, 6)
    relay_far(Q)
    for slot in (1, 3, 0, 4):
        recv(stat.at[slot], stat_sem.at[slot], live(slot))
    collect_some(4, lambda i: (1 + 2 * lax.rem(i, 2), lax.div(i, 2)), False)

    def mix_sum(side):
        for i in range(3):
            recv(mix_recv.at[i, side], mix_sem.at[i, side])
        return mix_keep[side] + sum(mix_recv[i, side].astype(F32) for i in range(3))

    mix_tail[...] = mix_sum(0).astype(BF)
    send(mix_tail, mix_land, mix_sem.at[3, 0], across)
    query_some(6, 10)
    stage[0] = dq_acc[...].T.astype(BF)
    send(stage.at[0, theirs], dq_out.at[:, my_head], out_sem.at[0], pair)
    dq_out[:, my_head] = stage[0, mine]
    dw_recv[z] = dw_send[z]
    for plane in range(NZ):
        recv(dw_recv.at[plane], dwz_sem.at[plane], z != plane)
    part = dw_recv[0].astype(F32)
    for plane in range(1, NZ):
        part = part + dw_recv[plane].astype(F32)
    dw_part[...] = part.T.astype(BF)

    def cut(yy, k):
        return pl.ds(pl.multiple_of((yy * 2 + k) * 32, 32), 32)

    for step in range(NY):
        yy = lax.rem(y + step, NY)
        for far in range(2):
            k = core if far == 0 else other
            if step == 0 and far == 0:
                dw_land[0, core] = dw_part[cut(yy, k)]
            else:
                send(dw_part.at[cut(yy, k)], dw_land.at[step, core], dwy_sem.at[step, core],
                     at(z * NY + yy, k))

    relay_last(Q)
    relay_end(G)
    collect_some(4, lambda i: (4 * lax.rem(i, 2), lax.div(i, 2)), True)
    for i, (total_ref, out_ref) in enumerate(((dk_acc, dk_out), (dv_acc, dv_out))):
        stage[1 + i] = total_ref[...].astype(BF)
        send(stage.at[1 + i, theirs], out_ref.at[:, my_head], out_sem.at[1 + i], pair)
        out_ref[:, my_head] = stage[1 + i, mine]

    total = mix_sum(1)
    recv(mix_land, mix_sem.at[3, 0])
    mixed_out[...] = (total + mix_land[...].astype(F32)).astype(BF)
    for step in range(NY):
        for far in range(2):
            k = core if far == 0 else other
            if not (step == 0 and far == 0):
                recv(dw_land.at[step, k], dwy_sem.at[step, k])
    for k in range(2):
        dw_out[:, k * HD:(k + 1) * HD] = sum(dw_land[s, k].astype(F32) for s in range(NY)).astype(BF)
    for i, out_ref in enumerate((dq_out, dk_out, dv_out)):
        recv(out_ref.at[:, their_head], out_sem.at[i])
    assert len(sent) <= SENDS
    for make, cond in sent:
        when(cond, lambda: make().wait_send())


def finish(*refs):
    ins, outs, sem = refs[:5], refs[5:10], refs[10]
    copies = [pltpu.make_async_copy(a, b, sem.at[i]) for i, (a, b) in enumerate(zip(ins, outs))]
    for copy in copies:
        copy.start()
    for copy in copies:
        copy.wait()


SENDS = 136


def body(queries, keys, values, out_grad, out_weight):
    dma = pltpu.SemaphoreType.DMA
    vmem = pltpu.VMEM
    results = pl.pallas_call(
        kernel,
        out_shape=(*(pltpu.VMEM((HALF, HALF), BF) for _ in range(4)), pltpu.VMEM((32, HALF), BF)),
        in_specs=[pl.BlockSpec(memory_space=pltpu.HBM)] * 5,
        out_specs=[pl.BlockSpec(memory_space=pltpu.VMEM)] * 5,
        scratch_shapes=[
            vmem((HALF, HALF), BF),
            vmem((HALF, HALF), BF),
            vmem((HALF, HALF), BF),
            vmem((HALF, HALF), BF),
            vmem((HALF, 2048), BF),
            vmem((4, 5, TOK, HD), BF),
            vmem((8, HALF, HALF), BF),
            vmem((8, HALF, HALF), BF),
            vmem((5, 8, HD), F32),
            vmem((10, HALF, TOK), F32),
            vmem((1, TOK), F32),
            vmem((1, TOK), F32),
            vmem((HD, TOK), F32),
            vmem((HD, TOK), BF),
            vmem((TOK, HD), BF),
            vmem((HALF, HALF), BF),
            vmem((HD, TOK), F32),
            vmem((TOK, HD), F32),
            vmem((TOK, HD), F32),
            vmem((3, TOK, HD), BF),
            vmem((3, 2, HALF, HALF), BF),
            vmem((3, 2, HALF, HALF), BF),
            vmem((2, HALF, HALF), F32),
            vmem((HALF, HALF), BF),
            vmem((HALF, HALF), BF),
            vmem((NZ, HD, HALF), BF),
            vmem((NZ, HD, HALF), BF),
            vmem((HALF, HD), BF),
            vmem((NY, 2, 32, HD), BF),
            vmem((2, HALF, HD), BF),
            dma((5,)),
            dma((SENDS,)),
            dma((4, 5, 2)),
            dma((5,)),
            dma((8,)),
            dma((8,)),
            dma((5,)),
            dma((4, 2)),
            dma((NZ,)),
            dma((NY, 2)),
            dma((3,)),
            dma((2,)),
            pltpu.SemaphoreType.REGULAR((2,)),
        ],
        compiler_params=pltpu.CompilerParams(
            collective_id=0, has_side_effects=True, vmem_limit_bytes=60 * 2**20
        ),
    )(queries, keys, values, out_grad, out_weight)
    shapes = [jax.ShapeDtypeStruct(r.shape, BF) for r in results]
    *results, dw = pl.pallas_call(
        finish,
        out_shape=shapes,
        in_specs=[pl.BlockSpec(memory_space=pltpu.VMEM)] * 5,
        out_specs=[pl.BlockSpec(memory_space=pltpu.HBM)] * 5,
        scratch_shapes=[dma((5,))],
    )(*(pltpu.with_memory_space_constraint(r, pltpu.VMEM) for r in results))
    return (*results, dw.T)


def solution(mesh):
    placed = (
        P("frames", "heads"),
        P("frames", "heads"),
        P("frames", "heads"),
        P("frames", "heads"),
        P("heads", None),
    )
    return jax.shard_map(
        body,
        mesh=mesh,
        in_specs=placed,
        out_specs=(
            P("frames", "heads"),
            P("frames", "heads"),
            P("frames", "heads"),
            P("frames", "heads"),
            P("heads", "frames"),
        ),
        check_vma=False,
    )
```
